8 devices in a mesh: rep: 1 (over z), dp: 8 (over x, y, core).
Axes of the slice: x: 2, y: 2, z: 1, core: 2. Of those that a mesh axis runs over, the one named last changes fastest.
Arguments:
- g_w_gate: bfloat16 [8, 2, 1152, 4608], P(('rep', 'dp'))
- g_w_up: bfloat16 [8, 2, 1152, 4608], P(('rep', 'dp'))
- g_w_down: bfloat16 [8, 2, 4608, 1152], P(('rep', 'dp'))
- w_gate: bfloat16 [2, 1152, 4608], replicated
- w_up: bfloat16 [2, 1152, 4608], replicated
- w_down: bfloat16 [2, 4608, 1152], replicated
- m_w_gate: float32 [2, 1152, 4608], P(None, 'dp')
- m_w_up: float32 [2, 1152, 4608], P(None, 'dp')
- m_w_down: float32 [2, 4608, 1152], P(None, 'dp')
- v_w_gate: float32 [2, 1152, 4608], P(None, 'dp')
- v_w_up: float32 [2, 1152, 4608], P(None, 'dp')
- v_w_down: float32 [2, 4608, 1152], P(None, 'dp')
Outputs:
- output 1: bfloat16 [2, 1152, 4608], P('rep')
- output 2: bfloat16 [2, 1152, 4608], P('rep')
- output 3: bfloat16 [2, 4608, 1152], P('rep')
- output 4: float32 [2, 1152, 4608], P('rep', 'dp')
- output 5: float32 [2, 1152, 4608], P('rep', 'dp')
- output 6: float32 [2, 4608, 1152], P('rep', 'dp')
- output 7: float32 [2, 1152, 4608], P('rep', 'dp')
- output 8: float32 [2, 1152, 4608], P('rep', 'dp')
- output 9: float32 [2, 4608, 1152], P('rep', 'dp')
All inputs are finite; a program needn't handle non-finite values.
Results may differ from the reference program's by a relative error of at most 0.022.
Values are sent between devices in bfloat16 or wider.
A program may use at most 2 GiB of HBM per device.

```python
import jax
import jax.numpy as jnp
from jax import lax

DEVICES = 8
D = 1152
FF = 4608
LAYERS = 2
NAMES = ("w_gate", "w_up", "w_down")
SHAPES = {"w_gate": (LAYERS, D, FF), "w_up": (LAYERS, D, FF), "w_down": (LAYERS, FF, D)}


def setup_inputs(seed: int = 0, part: int = 0) -> dict:
    kz, *keys = jax.random.split(jax.random.key(seed), 1 + 5 * len(NAMES))
    loud = 2.0 ** jax.random.uniform(kz, (), jnp.float32, -1.0, 1.0)
    drawn = {}
    for name, key, both in zip(NAMES, keys[:3], keys[3:6], strict=True):
        own = jax.random.normal(jax.random.fold_in(key, part), (DEVICES, *SHAPES[name]), jnp.float32)
        shared = jax.random.normal(jax.random.fold_in(both, part), SHAPES[name], jnp.float32)
        drawn["g_" + name] = (loud * (0.7 * shared / DEVICES + 0.7 * own * DEVICES**-0.5)).astype(jnp.bfloat16)
    for name, key in zip(NAMES, keys[6:9], strict=True):
        drawn[name] = (jax.random.normal(key, SHAPES[name], jnp.float32) * SHAPES[name][1] ** -0.5).astype(jnp.bfloat16)
    for name, key in zip(NAMES, keys[9:12], strict=True):
        drawn["m_" + name] = loud * 0.5 * jax.random.normal(key, SHAPES[name], jnp.float32)
    for name, key in zip(NAMES, keys[12:15], strict=True):
        drawn["v_" + name] = loud * loud * jax.random.uniform(key, SHAPES[name], jnp.float32, 0.5, 1.5)
    return drawn


def adamw(w, m, v, g):
    m = 0.9 * m + 0.1 * g
    v = 0.95 * v + 0.05 * g * g
    step = m * lax.rsqrt(v + 1e-8) + 0.1 * w
    return (w - 0.02 * step).astype(jnp.bfloat16), m, v


def reference(g_w_gate, g_w_up, g_w_down, w_gate, w_up, w_down, m_w_gate, m_w_up, m_w_down, v_w_gate, v_w_up, v_w_down):
    def total(terms):
        return lax.scan(lambda so_far, term: (so_far + term.astype(jnp.float32), None), jnp.zeros(terms.shape[1:], jnp.float32), terms)[0]

    gradients = [total(terms).astype(jnp.bfloat16).astype(jnp.float32) for terms in (g_w_gate, g_w_up, g_w_down)]
    new = [
        adamw(w.astype(jnp.float32), m, v, g)
        for w, m, v, g in zip((w_gate, w_up, w_down), (m_w_gate, m_w_up, m_w_down), (v_w_gate, v_w_up, v_w_down), gradients, strict=True)
    ]
    return tuple(one[which] for which in range(3) for one in new)
```

```python
import functools

import jax
import jax.numpy as jnp
from jax import lax
from jax.experimental import pallas as pl
from jax.experimental.pallas import tpu as pltpu
from jax.sharding import PartitionSpec as P

MESH = pl.DeviceIdType.MESH
LAG = 2


def chunk_list(rows_of, weights, layers):
    out = []
    pairs = [(w, l) for w in range(weights) for l in range(layers)]
    for i, (w, l) in enumerate(pairs):
        unit = rows_of[w] // 9
        parts = [3, 3, 3]
        if i == 0:
            parts = [1, 2, 3, 3]
        if i == len(pairs) - 1:
            parts = [3, 3, 2, 1]
        first = 0
        for p in parts:
            out.append((w, l, first * unit, p * unit))
            first += p
    return out


class Copies:
    def __init__(self, send, recv, local):
        self.send, self.recv, self.local = send, recv, local
        self.ids, self.nlocal, self.remote, self.here = {}, 0, {}, {}

    def start_remote(self, key, src, dst, peer):
        n = self.ids.setdefault(key, len(self.ids))
        c = pltpu.make_async_remote_copy(src, dst, self.send.at[n], self.recv.at[n], device_id={"dp": peer}, device_id_type=MESH)
        c.start()
        self.remote[key] = [c, True, True]

    def wait_recv(self, key):
        c = self.remote[key]
        assert c[2]
        c[0].wait_recv()
        c[2] = False

    def wait_send(self, key):
        c = self.remote.get(key)
        if c is not None and c[1]:
            c[0].wait_send()
            c[1] = False

    def start(self, key, slot, src, dst):
        c = pltpu.make_async_copy(src, dst, self.local.at[slot])
        c.start()
        self.here[key] = c

    def wait(self, key):
        c = self.here.pop(key, None)
        if c is not None:
            c.wait()

    def drain(self):
        for c in self.here.values():
            c.wait()
        for c in self.remote.values():
            if c[1]:
                c[0].wait_send()
            if c[2]:
                c[0].wait_recv()


OWN, PART, SENDA, KEEPA, RECVA, SENDB, KEEPB, RECVB, GOUT, WNEW = 2, 2, 3, 3, 1, 2, 3, 1, 2, 4
L_OWN, L_PART, L_RECVA, L_RECVB, L_M, L_V, L_W, L_G, L_WN, L_ALL = 0, 2, 4, 5, 6, 7, 8, 9, 11, 15


def body(chunks, group, kinds, *refs):
    g, w, m, v = refs[0:3], refs[3:6], refs[6:9], refs[9:12]
    wn, gs, pland, aland, bland = refs[12:15], refs[15:18], refs[18:21], refs[21:24], refs[24:27]
    bufs = (refs[27:40], refs[40:53])
    send, recv, local = refs[53:56]

    me = lax.axis_index("dp")
    x, y, c = me // 4, (me // 2) % 2, me % 2
    xy = 2 * x + y
    peer_x, peer_y, mate = me + 4 - 8 * x, me + 2 - 4 * y, me + 1 - 2 * c
    peer_a = peer_x + c * (peer_y - peer_x)
    peer_b = peer_y + c * (peer_x - peer_y)
    xy_x, xy_y = xy + 2 - 4 * x, xy + 1 - 2 * y
    xy_a = xy_x + c * (xy_y - xy_x)
    xy_b = xy_y + c * (xy_x - xy_y)
    xy_ab = 3 - xy

    barrier = pltpu.get_barrier_semaphore()
    for peer in (peer_a, peer_b, mate):
        pl.semaphore_signal(barrier, inc=1, device_id={"dp": peer}, device_id_type=MESH)
    pl.semaphore_wait(barrier, 3)

    cp = Copies(send, recv, local)
    count = len(chunks)

    def at(k):
        wi, layer, first, rows = chunks[k]
        return wi, layer, pl.ds(first, rows), rows, bufs[kinds[wi]], group[wi]

    def exchange(k):
        wi, layer, rs, _, _, _ = at(k)
        cp.start_remote(("d", k), g[wi].at[layer, :, 1 - c, rs, :], pland[wi].at[layer, :, rs, :], mate)

    def load_terms(k):
        wi, layer, rs, rows, b, _ = at(k)
        cp.wait_recv(("d", k))
        cp.start(("own", k), L_OWN + k % OWN, g[wi].at[layer, :, c, rs, :], b[0].at[k % OWN, :, pl.ds(0, rows), :])
        cp.start(("part", k), L_PART + k % PART, pland[wi].at[layer, :, rs, :], b[1].at[k % PART, :, pl.ds(0, rows), :])

    def load_a(k):
        wi, layer, rs, rows, b, _ = at(k)
        cp.wait_recv(("a", k))
        cp.start(("recva", k), L_RECVA, aland[wi].at[layer, :, rs, :], b[4].at[:, pl.ds(0, rows), :])

    def load_b(k):
        wi, layer, rs, rows, b, _ = at(k)
        top = pl.ds(0, rows)
        cp.start(("m", k), L_M, m[wi].at[layer, rs, :], b[8].at[top, :])
        cp.start(("v", k), L_V, v[wi].at[layer, rs, :], b[9].at[top, :])
        cp.start(("w", k), L_W, w[wi].at[layer, xy, c, rs, :], b[10].at[top, :])
        cp.wait_recv(("b", k))
        cp.start(("recvb", k), L_RECVB, bland[wi].at[layer, rs, :], b[7].at[top, :])

    def forward_b(k):
        wi, layer, rs, _, _, _ = at(k)
        cp.wait_recv(("gb", k))
        part = wn[wi].at[layer, xy_b, c, rs, :]
        cp.start_remote(("gab", k), part, part, peer_a)
        cp.start_remote(("mb", k), part, part, mate)

    def forward_a(k):
        wi, layer, rs, _, _, _ = at(k)
        for kind, place in (("ga", xy_a), ("gab", xy_ab)):
            cp.wait_recv((kind, k))
            part = wn[wi].at[layer, place, c, rs, :]
            cp.start_remote(("m" + kind, k), part, part, mate)

    def sum_mates(k):
        wi, layer, rs, rows, b, step = at(k)
        own, part, senda, keepa = b[0], b[1], b[2], b[3]
        cp.wait(("own", k))
        cp.wait(("part", k))
        cp.wait_send(("a", k - SENDA))
        so, sp, ss, sk = k % OWN, k % PART, k % SENDA, k % KEEPA

        def sums(i, _):
            r = pl.ds(pl.multiple_of(i * step, step), step)
            for j, place in ((0, xy_ab), (1, xy_a)):
                t = own[so, place, r, :].astype(jnp.float32) + part[sp, place, r, :].astype(jnp.float32)
                senda[ss, j, r, :] = t.astype(jnp.bfloat16)
            for j, place in ((0, xy_b), (1, xy)):
                t = own[so, place, r, :].astype(jnp.float32) + part[sp, place, r, :].astype(jnp.float32)
                keepa[sk, j, r, :] = t
            return 0

        lax.fori_loop(0, rows // step, sums, 0)
        cp.start_remote(("a", k), senda.at[ss, :, pl.ds(0, rows), :], aland[wi].at[layer, :, rs, :], peer_a)

    def sum_a(k):
        wi, layer, rs, rows, b, step = at(k)
        keepa, recva, sendb, keepb = b[3], b[4], b[5], b[6]
        cp.wait(("recva", k))
        cp.wait_send(("b", k - SENDB))
        sk, ss, sb = k % KEEPA, k % SENDB, k % KEEPB

        def sums(i, _):
            r = pl.ds(pl.multiple_of(i * step, step), step)
            sendb[ss, r, :] = (keepa[sk, 0, r, :] + recva[0, r, :].astype(jnp.float32)).astype(jnp.bfloat16)
            keepb[sb, r, :] = keepa[sk, 1, r, :] + recva[1, r, :].astype(jnp.float32)
            return 0

        lax.fori_loop(0, rows // step, sums, 0)
        cp.start_remote(("b", k), sendb.at[ss, pl.ds(0, rows), :], bland[wi].at[layer, rs, :], peer_b)

    def update(k):
        wi, layer, rs, rows, b, step = at(k)
        keepb, recvb, mb, vb, wb, gb, nb = b[6], b[7], b[8], b[9], b[10], b[11], b[12]
        for kind in ("recvb", "m", "v", "w"):
            cp.wait((kind, k))
        cp.wait(("gout", k - GOUT))
        cp.wait(("wout", k - WNEW))
        for kind in ("gb", "ga", "mo"):
            cp.wait_send((kind, k - WNEW))
        sb, sg, sn = k % KEEPB, k % GOUT, k % WNEW

        def new(i, _):
            r = pl.ds(pl.multiple_of(i * step, step), step)
            total = (keepb[sb, r, :] + recvb[r, :].astype(jnp.float32)).astype(jnp.bfloat16)
            gb[sg, r, :] = total
            gf = total.astype(jnp.float32)
            m1 = 0.9 * mb[r, :] + 0.1 * gf
            v1 = 0.95 * vb[r, :] + 0.05 * gf * gf
            w0 = wb[r, :].astype(jnp.float32)
            nb[sn, r, :] = (w0 - 0.02 * (m1 * lax.rsqrt(v1 + 1e-8) + 0.1 * w0)).astype(jnp.bfloat16)
            return 0

        lax.fori_loop(0, rows // step, new, 0)
        top = pl.ds(0, rows)
        src, dst = nb.at[sn, top, :], wn[wi].at[layer, xy, c, rs, :]
        cp.start_remote(("gb", k), src, dst, peer_b)
        cp.start_remote(("ga", k), src, dst, peer_a)
        cp.start_remote(("mo", k), src, dst, mate)
        cp.start(("wout", k), L_WN + sn, src, dst)
        cp.start(("gout", k), L_G + sg, gb.at[sg, top, :], gs[wi].at[layer, rs, :])

    def when(k, f):
        if 0 <= k < count:
            f(k)

    when(0, exchange)
    when(1, exchange)
    when(0, load_terms)
    for s in range(count + 4 * LAG):
        when(s + 2, exchange)
        when(s + 1, load_terms)
        when(s - LAG, load_a)
        when(s - 2 * LAG, load_b)
        when(s - 3 * LAG, forward_b)
        when(s - 4 * LAG, forward_a)
        when(s, sum_mates)
        when(s - LAG, sum_a)
        when(s - 2 * LAG, update)
    cp.drain()


def solution(mesh):
    n = mesh.shape["dp"]

    def step(*arrays):
        terms, weights, m, v = (arrays[i : i + 3] for i in (0, 3, 6, 9))
        layers = weights[0].shape[0]
        rows = [one.shape[1] for one in m]
        cols = [one.shape[2] for one in m]
        kinds, shapes = [], []
        for one in zip(rows, cols):
            if one not in shapes:
                shapes.append(one)
            kinds.append(shapes.index(one))
        group = [r // 9 for r in rows]
        chunks = chunk_list(rows, 3, layers)

        def blocks(a, r):
            return a.reshape(layers, n // 2, 2, r, a.shape[-1])

        gb = [blocks(t[0], r) for t, r in zip(terms, rows)]
        wb = [blocks(t, r) for t, r in zip(weights, rows)]
        bf, f32 = jnp.bfloat16, jnp.float32
        out = [jax.ShapeDtypeStruct((layers, n // 2, 2, r, q), bf) for r, q in zip(rows, cols)]
        out += [jax.ShapeDtypeStruct((layers, r, q), bf) for r, q in zip(rows, cols)]
        out += [jax.ShapeDtypeStruct((layers, n // 2, r, q), bf) for r, q in zip(rows, cols)]
        out += [jax.ShapeDtypeStruct((layers, 2, r, q), bf) for r, q in zip(rows, cols)]
        out += [jax.ShapeDtypeStruct((layers, r, q), bf) for r, q in zip(rows, cols)]
        scratch = []
        for r, q in shapes:
            u = (r // 3, q)
            scratch += [
                pltpu.VMEM((OWN, n // 2, *u), bf),
                pltpu.VMEM((PART, n // 2, *u), bf),
                pltpu.VMEM((SENDA, 2, *u), bf),
                pltpu.VMEM((KEEPA, 2, *u), f32),
                pltpu.VMEM((2, *u), bf),
                pltpu.VMEM((SENDB, *u), bf),
                pltpu.VMEM((KEEPB, *u), f32),
                pltpu.VMEM(u, bf),
                pltpu.VMEM(u, f32),
                pltpu.VMEM(u, f32),
                pltpu.VMEM(u, bf),
                pltpu.VMEM((GOUT, *u), bf),
                pltpu.VMEM((WNEW, *u), bf),
            ]
        copies = 10 * len(chunks)
        scratch += [pltpu.SemaphoreType.DMA((copies,)), pltpu.SemaphoreType.DMA((copies,)), pltpu.SemaphoreType.DMA((L_ALL,))]
        hbm = pl.BlockSpec(memory_space=pl.ANY)
        res = pl.pallas_call(
            functools.partial(body, chunks, group, kinds),
            out_shape=out,
            in_specs=[hbm] * 12,
            out_specs=[hbm] * len(out),
            scratch_shapes=scratch,
            compiler_params=pltpu.CompilerParams(collective_id=0, has_side_effects=True, vmem_limit_bytes=60 * 2**20),
            name="sum_step_gather",
        )(*gb, *wb, *m, *v)
        whole = [one.reshape(w.shape) for one, w in zip(res[0:3], weights)]
        total = [one.astype(f32) for one in res[3:6]]
        new_m = [0.9 * a + 0.1 * t for a, t in zip(m, total)]
        new_v = [0.95 * a + 0.05 * t * t for a, t in zip(v, total)]
        return (*whole, *new_m, *new_v)

    all_of, cut = P(None, None, None), P(None, "dp", None)
    return jax.shard_map(
        step,
        mesh=mesh,
        in_specs=(P(("rep", "dp"), None, None, None),) * 3 + (all_of,) * 3 + (cut,) * 6,
        out_specs=(P("rep", None, None),) * 3 + (P("rep", "dp", None),) * 6,
        check_vma=False,
    )
```

```python
import functools

import jax
import jax.numpy as jnp
from jax import lax
from jax.experimental import pallas as pl
from jax.experimental.pallas import tpu as pltpu
from jax.sharding import PartitionSpec as P


MESH = pl.DeviceIdType.MESH
LAG = 2


def chunk_list(rows_of, weights, layers):
    out = []
    pairs = [(w, l) for w in range(weights) for l in range(layers)]
    for i, (w, l) in enumerate(pairs):
        unit = rows_of[w] // 9
        parts = [3, 3, 3]
        if i == 0:
            parts = [1, 2, 3, 3]
        if i == len(pairs) - 1:
            parts = [3, 3, 2, 1]
        first = 0
        for p in parts:
            out.append((w, l, first * unit, p * unit))
            first += p
    return out


class Copies:
    def __init__(self, send, recv, local):
        self.send, self.recv, self.local = send, recv, local
        self.ids, self.nlocal, self.remote, self.here = {}, 0, {}, {}

    def start_remote(self, key, src, dst, peer):
        n = self.ids.setdefault(key, len(self.ids))
        c = pltpu.make_async_remote_copy(src, dst, self.send.at[n], self.recv.at[n], device_id={"dp": peer}, device_id_type=MESH)
        c.start()
        self.remote[key] = [c, True, True]

    def wait_recv(self, key):
        c = self.remote[key]
        assert c[2]
        c[0].wait_recv()
        c[2] = False

    def wait_send(self, key):
        c = self.remote.get(key)
        if c is not None and c[1]:
            c[0].wait_send()
            c[1] = False

    def start(self, key, slot, src, dst):
        c = pltpu.make_async_copy(src, dst, self.local.at[slot])
        c.start()
        self.here[key] = c

    def wait(self, key):
        c = self.here.pop(key, None)
        if c is not None:
            c.wait()

    def drain(self):
        for c in self.here.values():
            c.wait()
        for c in self.remote.values():
            if c[1]:
                c[0].wait_send()
            if c[2]:
                c[0].wait_recv()


OWN, PART, SENDA, KEEPA, SENDB, KEEPB, GOUT, WNEW = 2, 2, 3, 3, 2, 3, 2, 4
L_OWN, L_PART, L_RECVA, L_RECVB, L_M, L_V, L_W, L_G, L_WN, L_ALL = 0, 2, 4, 5, 6, 7, 8, 9, 11, 15


def body(chunks, group, kinds, outside, *refs):
    g, w, m, v = refs[0:3], refs[3:6], refs[6:9], refs[9:12]
    wn, gs, pland, aland, bland = refs[12:15], refs[15:18], refs[18:21], refs[21:24], refs[24:27]
    bufs = (refs[27:40], refs[40:53])
    send, recv, local = refs[53:56]

    me = lax.axis_index("dp")
    x, y, c = me // 4, (me // 2) % 2, me % 2
    xy = 2 * x + y
    peer_x, peer_y, mate = me + 4 - 8 * x, me + 2 - 4 * y, me + 1 - 2 * c
    peer_a = peer_x + c * (peer_y - peer_x)
    peer_b = peer_y + c * (peer_x - peer_y)
    xy_x, xy_y = xy + 2 - 4 * x, xy + 1 - 2 * y
    xy_a = xy_x + c * (xy_y - xy_x)
    xy_b = xy_y + c * (xy_x - xy_y)
    xy_ab = 3 - xy

    barrier = pltpu.get_barrier_semaphore()
    for peer in (peer_a, peer_b, mate):
        pl.semaphore_signal(barrier, inc=1, device_id={"dp": peer}, device_id_type=MESH)
    pl.semaphore_wait(barrier, 3)

    cp = Copies(send, recv, local)
    count = len(chunks)

    def at(k):
        wi, layer, first, rows = chunks[k]
        return wi, layer, pl.ds(first, rows), rows, bufs[kinds[wi]], group[wi]

    def exchange(k):
        wi, layer, rs, _, _, _ = at(k)
        cp.start_remote(("d", k), g[wi].at[layer, :, 1 - c, rs, :], pland[wi].at[layer, :, rs, :], mate)

    def load_terms(k):
        wi, layer, rs, rows, b, _ = at(k)
        cp.wait_recv(("d", k))
        cp.start(("own", k), L_OWN + k % OWN, g[wi].at[layer, :, c, rs, :], b[0].at[k % OWN, :, pl.ds(0, rows), :])
        cp.start(("part", k), L_PART + k % PART, pland[wi].at[layer, :, rs, :], b[1].at[k % PART, :, pl.ds(0, rows), :])

    def load_a(k):
        wi, layer, rs, rows, b, _ = at(k)
        cp.wait_recv(("a", k))
        cp.start(("recva", k), L_RECVA, aland[wi].at[layer, :, rs, :], b[4].at[:, pl.ds(0, rows), :])

    def load_b(k):
        wi, layer, rs, rows, b, _ = at(k)
        top = pl.ds(0, rows)
        cp.start(("m", k), L_M, m[wi].at[layer, rs, :], b[8].at[top, :])
        cp.start(("v", k), L_V, v[wi].at[layer, rs, :], b[9].at[top, :])
        cp.start(("w", k), L_W, w[wi].at[layer, xy, c, rs, :], b[10].at[top, :])
        cp.wait_recv(("b", k))
        cp.start(("recvb", k), L_RECVB, bland[wi].at[layer, rs, :], b[7].at[top, :])

    def forward_b(k):
        wi, layer, rs, _, _, _ = at(k)
        cp.wait_recv(("gb", k))
        part = wn[wi].at[layer, xy_b, c, rs, :]
        cp.start_remote(("gab", k), part, part, peer_a)
        cp.start_remote(("mb", k), part, part, mate)

    def forward_a(k):
        wi, layer, rs, _, _, _ = at(k)
        for kind, place in (("ga", xy_a), ("gab", xy_ab)):
            cp.wait_recv((kind, k))
            part = wn[wi].at[layer, place, c, rs, :]
            cp.start_remote(("m" + kind, k), part, part, mate)

    def sum_mates(k):
        wi, layer, rs, rows, b, step = at(k)
        own, part, senda, keepa = b[0], b[1], b[2], b[3]
        cp.wait(("own", k))
        cp.wait(("part", k))
        cp.wait_send(("a", k - SENDA))
        so, sp, ss, sk = k % OWN, k % PART, k % SENDA, k % KEEPA

        def sums(i, _):
            r = pl.ds(pl.multiple_of(i * step, step), step)
            for j, place in ((0, xy_ab), (1, xy_a)):
                t = own[so, place, r, :].astype(jnp.float32) + part[sp, place, r, :].astype(jnp.float32)
                senda[ss, j, r, :] = t.astype(jnp.bfloat16)
            for j, place in ((0, xy_b), (1, xy)):
                t = own[so, place, r, :].astype(jnp.float32) + part[sp, place, r, :].astype(jnp.float32)
                keepa[sk, j, r, :] = t
            return 0

        lax.fori_loop(0, rows // step, sums, 0)
        cp.start_remote(("a", k), senda.at[ss, :, pl.ds(0, rows), :], aland[wi].at[layer, :, rs, :], peer_a)

    def sum_a(k):
        wi, layer, rs, rows, b, step = at(k)
        keepa, recva, sendb, keepb = b[3], b[4], b[5], b[6]
        cp.wait(("recva", k))
        cp.wait_send(("b", k - SENDB))
        sk, ss, sb = k % KEEPA, k % SENDB, k % KEEPB

        def sums(i, _):
            r = pl.ds(pl.multiple_of(i * step, step), step)
            sendb[ss, r, :] = (keepa[sk, 0, r, :] + recva[0, r, :].astype(jnp.float32)).astype(jnp.bfloat16)
            keepb[sb, r, :] = keepa[sk, 1, r, :] + recva[1, r, :].astype(jnp.float32)
            return 0

        lax.fori_loop(0, rows // step, sums, 0)
        cp.start_remote(("b", k), sendb.at[ss, pl.ds(0, rows), :], bland[wi].at[layer, rs, :], peer_b)

    def update(k):
        wi, layer, rs, rows, b, step = at(k)
        inside = wi not in outside
        keepb, recvb, mb, vb, wb, gb, nb = b[6], b[7], b[8], b[9], b[10], b[11], b[12]
        for kind in ("recvb", "m", "v", "w"):
            cp.wait((kind, k))
        cp.wait(("gout", k - GOUT))
        cp.wait(("wout", k - WNEW))
        for kind in ("gb", "ga", "mo"):
            cp.wait_send((kind, k - WNEW))
        sb, sg, sn = k % KEEPB, k % GOUT, k % WNEW

        def new(i, _):
            r = pl.ds(pl.multiple_of(i * step, step), step)
            total = (keepb[sb, r, :] + recvb[r, :].astype(jnp.float32)).astype(jnp.bfloat16)
            gb[sg, r, :] = total
            gf = total.astype(jnp.float32)
            m1 = 0.9 * mb[r, :] + 0.1 * gf
            v1 = 0.95 * vb[r, :] + 0.05 * gf * gf
            w0 = wb[r, :].astype(jnp.float32)
            nb[sn, r, :] = (w0 - 0.02 * (m1 * lax.rsqrt(v1 + 1e-8) + 0.1 * w0)).astype(jnp.bfloat16)
            return 0

        lax.fori_loop(0, rows // step, new, 0)
        top = pl.ds(0, rows)
        src = nb.at[sn, top, :]
        if inside:
            dst = wn[wi].at[layer, xy, c, rs, :]
            cp.start_remote(("gb", k), src, dst, peer_b)
            cp.start_remote(("ga", k), src, dst, peer_a)
            cp.start_remote(("mo", k), src, dst, mate)
        else:
            dst = wn[wi].at[layer, rs, :]
        cp.start(("wout", k), L_WN + sn, src, dst)
        cp.start(("gout", k), L_G + sg, gb.at[sg, top, :], gs[wi].at[layer, rs, :])

    def when(k, f, gathers=False):
        if 0 <= k < count and not (gathers and chunks[k][0] in outside):
            f(k)

    when(0, exchange)
    when(1, exchange)
    when(0, load_terms)
    for s in range(count + 4 * LAG):
        when(s + 2, exchange)
        when(s + 1, load_terms)
        when(s - LAG, load_a)
        when(s - 2 * LAG, load_b)
        when(s - 3 * LAG, forward_b, True)
        when(s - 4 * LAG, forward_a, True)
        when(s, sum_mates)
        when(s - LAG, sum_a)
        when(s - 2 * LAG, update)
    cp.drain()


def copy_blocks(a):
    layers, places, cores, r, q = a.shape

    def kernel(src, dst):
        dst[...] = src[...]

    spec = pl.BlockSpec((None, None, None, r, q), lambda i, j, k: (i, j, k, 0, 0))
    return pl.pallas_call(
        kernel,
        out_shape=jax.ShapeDtypeStruct(a.shape, a.dtype),
        grid=(layers, places, cores),
        in_specs=[spec],
        out_specs=spec,
        cost_estimate=pl.CostEstimate(flops=4 * 10**9, bytes_accessed=4 * a.size, transcendentals=0),
        name="copy_blocks",
    )(a)


def place_blocks(pieces, places, n, into=None):
    layers, r, q = pieces[0].shape
    count = len(pieces) * layers

    def kernel(*refs):
        src = refs[: len(pieces)]
        dst, buf, sin, sout = refs[-4:]
        me = lax.axis_index("dp")
        x, y, c = me // 4, (me // 2) % 2, me % 2
        loads, stores = [], []
        for p in range(len(pieces)):
            xy, core = places[p](x, y, c)
            for l in range(layers):
                i = p * layers + l
                loads.append(pltpu.make_async_copy(src[p].at[l], buf.at[i], sin.at[i]))
                stores.append(pltpu.make_async_copy(buf.at[i], dst.at[l, xy, core], sout.at[i]))
        for one in loads:
            one.start()
        for one, two in zip(loads, stores):
            one.wait()
            two.start()
        for two in stores:
            two.wait()

    hbm = pl.BlockSpec(memory_space=pl.ANY)
    more = [] if into is None else [into]
    return pl.pallas_call(
        kernel,
        out_shape=jax.ShapeDtypeStruct((layers, n // 2, 2, r, q), pieces[0].dtype),
        in_specs=[hbm] * (len(pieces) + len(more)),
        out_specs=hbm,
        scratch_shapes=[
            pltpu.VMEM((count, r, q), pieces[0].dtype),
            pltpu.SemaphoreType.DMA((count,)),
            pltpu.SemaphoreType.DMA((count,)),
        ],
        input_output_aliases={len(pieces): 0} if more else {},
        cost_estimate=pl.CostEstimate(flops=10**9, bytes_accessed=4 * count * r * q, transcendentals=0),
        name="place_blocks",
    )(*pieces, *more)


def gather(own, n):
    to_a = [(d, d ^ (2 if d % 2 else 4)) for d in range(n)]
    to_b = [(d, d ^ (4 if d % 2 else 2)) for d in range(n)]
    to_mate = [(d, d ^ 1) for d in range(n)]

    def send(what, pairs):
        return lax.ppermute(what, "dp", pairs)

    from_b = send(own, to_b)
    from_a = send(own, to_a)
    mate_own = send(own, to_mate)
    from_ab = send(from_b, to_a)
    mate_b = send(from_b, to_mate)
    mate_a = send(from_a, to_mate)
    mate_ab = send(from_ab, to_mate)

    def at_x(x, y):
        return 2 * (1 - x) + y

    def at_y(x, y):
        return 2 * x + 1 - y

    def a_of(x, y, c):
        return at_x(x, y) + c * (at_y(x, y) - at_x(x, y))

    def b_of(x, y, c):
        return at_y(x, y) + c * (at_x(x, y) - at_y(x, y))

    places = [
        lambda x, y, c: (2 * x + y, c),
        lambda x, y, c: (a_of(x, y, c), c),
        lambda x, y, c: (b_of(x, y, c), c),
        lambda x, y, c: (2 * x + y, 1 - c),
        lambda x, y, c: (b_of(x, y, c), 1 - c),
        lambda x, y, c: (a_of(x, y, c), 1 - c),
    ]
    first = place_blocks([own, from_a, from_b, mate_own, mate_a, mate_b], places, n)
    last = [lambda x, y, c: (3 - 2 * x - y, c), lambda x, y, c: (3 - 2 * x - y, 1 - c)]
    return place_blocks([from_ab, mate_ab], last, n, into=first)


def solution(mesh):
    n = mesh.shape["dp"]

    def inner(*arrays):
        terms, weights, m, v = (arrays[i : i + 3] for i in (0, 3, 6, 9))
        layers = weights[0].shape[0]
        rows = [one.shape[1] for one in m]
        cols = [one.shape[2] for one in m]
        kinds, shapes = [], []
        for one in zip(rows, cols):
            if one not in shapes:
                shapes.append(one)
            kinds.append(shapes.index(one))
        group = [r // 9 for r in rows]
        chunks = chunk_list(rows, 3, layers)

        def blocks(a, r):
            return a.reshape(layers, n // 2, 2, r, a.shape[-1])

        gb = [blocks(t[0], r) for t, r in zip(terms, rows)]
        wb = [blocks(t, r) for t, r in zip(weights, rows)]
        bf, f32 = jnp.bfloat16, jnp.float32
        out = [jax.ShapeDtypeStruct((layers, n // 2, 2, r, q), bf) for r, q in zip(rows[:2], cols)]
        out += [jax.ShapeDtypeStruct((layers, rows[2], cols[2]), bf)]
        out += [jax.ShapeDtypeStruct((layers, r, q), bf) for r, q in zip(rows, cols)]
        out += [jax.ShapeDtypeStruct((layers, n // 2, r, q), bf) for r, q in zip(rows, cols)]
        out += [jax.ShapeDtypeStruct((layers, 2, r, q), bf) for r, q in zip(rows, cols)]
        out += [jax.ShapeDtypeStruct((layers, r, q), bf) for r, q in zip(rows, cols)]
        scratch = []
        for r, q in shapes:
            u = (r // 3, q)
            scratch += [
                pltpu.VMEM((OWN, n // 2, *u), bf),
                pltpu.VMEM((PART, n // 2, *u), bf),
                pltpu.VMEM((SENDA, 2, *u), bf),
                pltpu.VMEM((KEEPA, 2, *u), f32),
                pltpu.VMEM((2, *u), bf),
                pltpu.VMEM((SENDB, *u), bf),
                pltpu.VMEM((KEEPB, *u), f32),
                pltpu.VMEM(u, bf),
                pltpu.VMEM(u, f32),
                pltpu.VMEM(u, f32),
                pltpu.VMEM(u, bf),
                pltpu.VMEM((GOUT, *u), bf),
                pltpu.VMEM((WNEW, *u), bf),
            ]
        copies = 10 * len(chunks)
        scratch += [pltpu.SemaphoreType.DMA((copies,)), pltpu.SemaphoreType.DMA((copies,)), pltpu.SemaphoreType.DMA((L_ALL,))]
        hbm = pl.BlockSpec(memory_space=pl.ANY)
        res = pl.pallas_call(
            functools.partial(body, chunks, group, kinds, (2,)),
            out_shape=out,
            in_specs=[hbm] * 12,
            out_specs=[hbm] * len(out),
            scratch_shapes=scratch,
            compiler_params=pltpu.CompilerParams(collective_id=0, has_side_effects=True, vmem_limit_bytes=60 * 2**20),
            name="sum_step_gather",
        )(*gb, *wb, *m, *v)
        whole = [copy_blocks(one) for one in res[0:2]]
        whole += [gather(res[2], n)]
        whole = [one.reshape(w.shape) for one, w in zip(whole, weights)]
        total = [one.astype(f32) for one in res[3:6]]
        new_m = [0.9 * a + 0.1 * t for a, t in zip(m, total)]
        new_v = [0.95 * a + 0.05 * t * t for a, t in zip(v, total)]
        return (*whole, *new_m, *new_v)

    all_of, cut = P(None, None, None), P(None, "dp", None)
    return jax.shard_map(
        inner,
        mesh=mesh,
        in_specs=(P(("rep", "dp"), None, None, None),) * 3 + (all_of,) * 3 + (cut,) * 6,
        out_specs=(P("rep", None, None),) * 3 + (P("rep", "dp", None),) * 6,
        check_vma=False,
    )
```

```python
import functools

import jax
import jax.numpy as jnp
from jax import lax
from jax.experimental import pallas as pl
from jax.experimental.pallas import tpu as pltpu
from jax.sharding import PartitionSpec as P


MESH = pl.DeviceIdType.MESH
LAG = 2


def chunk_list(rows_of, weights, layers):
    out = []
    pairs = [(w, l) for w in range(weights) for l in range(layers)]
    for i, (w, l) in enumerate(pairs):
        unit = rows_of[w] // 9
        parts = [3, 3, 3]
        if i == 0:
            parts = [1, 2, 3, 3]
        if i == len(pairs) - 1:
            parts = [3, 3, 2, 1]
        first = 0
        for p in parts:
            out.append((w, l, first * unit, p * unit))
            first += p
    return out


class Copies:
    def __init__(self, send, recv, local):
        self.send, self.recv, self.local = send, recv, local
        self.ids, self.nlocal, self.remote, self.here = {}, 0, {}, {}

    def start_remote(self, key, src, dst, peer):
        n = self.ids.setdefault(key, len(self.ids))
        c = pltpu.make_async_remote_copy(src, dst, self.send.at[n], self.recv.at[n], device_id={"dp": peer}, device_id_type=MESH)
        c.start()
        self.remote[key] = [c, True, True]

    def wait_recv(self, key):
        c = self.remote[key]
        assert c[2]
        c[0].wait_recv()
        c[2] = False

    def wait_send(self, key):
        c = self.remote.get(key)
        if c is not None and c[1]:
            c[0].wait_send()
            c[1] = False

    def start(self, key, slot, src, dst):
        c = pltpu.make_async_copy(src, dst, self.local.at[slot])
        c.start()
        self.here[key] = c

    def wait(self, key):
        c = self.here.pop(key, None)
        if c is not None:
            c.wait()

    def drain(self):
        for c in self.here.values():
            c.wait()
        for c in self.remote.values():
            if c[1]:
                c[0].wait_send()
            if c[2]:
                c[0].wait_recv()


OWN, PART, SENDA, KEEPA, SENDB, KEEPB, GOUT, WNEW = 2, 2, 3, 3, 2, 3, 2, 4
L_OWN, L_PART, L_RECVA, L_RECVB, L_M, L_V, L_W, L_G, L_WN, L_AG, L_ALL = 0, 2, 4, 5, 6, 7, 8, 9, 11, 15, 19


def body(chunks, group, kinds, outside, firsts, *refs):
    g, w, m, v = refs[0:3], refs[3:6], refs[6:9], refs[9:12]
    own_block, own_pieces, refs = refs[12], refs[13 : 13 + len(firsts)], refs[:12] + refs[13 + len(firsts) :]
    wn, gs, pland, aland, bland = refs[12:14], refs[14:17], refs[17:20], refs[20:23], refs[23:26]
    bufs = (refs[26:39], refs[39:52])
    last_a, last_b, send, recv, local = refs[52:57]

    me = lax.axis_index("dp")
    x, y, c = me // 4, (me // 2) % 2, me % 2
    xy = 2 * x + y
    peer_x, peer_y, mate = me + 4 - 8 * x, me + 2 - 4 * y, me + 1 - 2 * c
    peer_a = peer_x + c * (peer_y - peer_x)
    peer_b = peer_y + c * (peer_x - peer_y)
    xy_x, xy_y = xy + 2 - 4 * x, xy + 1 - 2 * y
    xy_a = xy_x + c * (xy_y - xy_x)
    xy_b = xy_y + c * (xy_x - xy_y)
    xy_ab = 3 - xy

    barrier = pltpu.get_barrier_semaphore()
    for peer in (peer_a, peer_b, mate):
        pl.semaphore_signal(barrier, inc=1, device_id={"dp": peer}, device_id_type=MESH)
    pl.semaphore_wait(barrier, 3)

    cp = Copies(send, recv, local)
    count = len(chunks)

    def at(k):
        wi, layer, first, rows = chunks[k]
        return wi, layer, pl.ds(first, rows), rows, bufs[kinds[wi]], group[wi]

    def exchange(k):
        wi, layer, rs, _, _, _ = at(k)
        land = pland[wi].at[layer, :, rs, :]
        if k < PART:
            land = bufs[kinds[wi]][1].at[k, :, pl.ds(0, chunks[k][3]), :]
        cp.start_remote(("d", k), g[wi].at[layer, :, 1 - c, rs, :], land, mate)

    def load_terms(k):
        wi, layer, rs, rows, b, _ = at(k)
        cp.start(("own", k), L_OWN + k % OWN, g[wi].at[layer, :, c, rs, :], b[0].at[k % OWN, :, pl.ds(0, rows), :])
        cp.wait_recv(("d", k))
        if k >= PART:
            cp.start(("part", k), L_PART + k % PART, pland[wi].at[layer, :, rs, :], b[1].at[k % PART, :, pl.ds(0, rows), :])

    def load_a(k):
        wi, layer, rs, rows, b, _ = at(k)
        cp.wait_recv(("a", k))
        if k == count - 1:
            return
        cp.start(("recva", k), L_RECVA, aland[wi].at[layer, :, rs, :], b[4].at[:, pl.ds(0, rows), :])

    def load_b(k):
        wi, layer, rs, rows, b, _ = at(k)
        top = pl.ds(0, rows)
        cp.start(("m", k), L_M, m[wi].at[layer, rs, :], b[8].at[top, :])
        cp.start(("v", k), L_V, v[wi].at[layer, rs, :], b[9].at[top, :])
        cp.start(("w", k), L_W, w[wi].at[layer, xy, c, rs, :], b[10].at[top, :])
        cp.wait_recv(("b", k))
        if k < count - 1:
            cp.start(("recvb", k), L_RECVB, bland[wi].at[layer, rs, :], b[7].at[top, :])

    def forward_b(k):
        wi, layer, rs, _, _, _ = at(k)
        cp.wait_recv(("gb", k))
        part = wn[wi].at[layer, xy_b, c, rs, :]
        cp.start_remote(("gab", k), part, part, peer_a)
        cp.start_remote(("mb", k), part, part, mate)

    def forward_a(k):
        wi, layer, rs, _, _, _ = at(k)
        for kind, place in (("ga", xy_a), ("gab", xy_ab)):
            cp.wait_recv((kind, k))
            part = wn[wi].at[layer, place, c, rs, :]
            cp.start_remote(("m" + kind, k), part, part, mate)

    def sum_mates(k):
        wi, layer, rs, rows, b, step = at(k)
        own, part, senda, keepa = b[0], b[1], b[2], b[3]
        cp.wait(("own", k))
        cp.wait(("part", k))
        cp.wait_send(("a", k - SENDA))
        so, sp, ss, sk = k % OWN, k % PART, k % SENDA, k % KEEPA

        def sums(i, _):
            r = pl.ds(pl.multiple_of(i * step, step), step)
            for j, place in ((0, xy_ab), (1, xy_a)):
                t = own[so, place, r, :].astype(jnp.float32) + part[sp, place, r, :].astype(jnp.float32)
                senda[ss, j, r, :] = t.astype(jnp.bfloat16)
            for j, place in ((0, xy_b), (1, xy)):
                t = own[so, place, r, :].astype(jnp.float32) + part[sp, place, r, :].astype(jnp.float32)
                keepa[sk, j, r, :] = t
            return 0

        lax.fori_loop(0, rows // step, sums, 0)
        cp.start_remote(("a", k), senda.at[ss, :, pl.ds(0, rows), :], last_a if k == count - 1 else aland[wi].at[layer, :, rs, :], peer_a)

    def sum_a(k):
        wi, layer, rs, rows, b, step = at(k)
        keepa, recva, sendb, keepb = b[3], b[4], b[5], b[6]
        cp.wait(("recva", k))
        cp.wait_send(("b", k - SENDB))
        sk, ss, sb = k % KEEPA, k % SENDB, k % KEEPB
        recva = last_a if k == count - 1 else recva

        def sums(i, _):
            r = pl.ds(pl.multiple_of(i * step, step), step)
            sendb[ss, r, :] = (keepa[sk, 0, r, :] + recva[0, r, :].astype(jnp.float32)).astype(jnp.bfloat16)
            keepb[sb, r, :] = keepa[sk, 1, r, :] + recva[1, r, :].astype(jnp.float32)
            return 0

        lax.fori_loop(0, rows // step, sums, 0)
        cp.start_remote(("b", k), sendb.at[ss, pl.ds(0, rows), :], last_b if k == count - 1 else bland[wi].at[layer, rs, :], peer_b)

    def update(k):
        wi, layer, rs, rows, b, step = at(k)
        inside = wi not in outside
        keepb, recvb, mb, vb, wb, gb, nb = b[6], b[7], b[8], b[9], b[10], b[11], b[12]
        for kind in ("recvb", "m", "v", "w"):
            cp.wait((kind, k))
        cp.wait(("gout", k - GOUT))
        cp.wait(("wout", k - WNEW))
        cp.wait(("again", k - WNEW))
        for kind in ("gb", "ga", "mo"):
            cp.wait_send((kind, k - WNEW))
        sb, sg, sn = k % KEEPB, k % GOUT, k % WNEW
        recvb = last_b if k == count - 1 else recvb

        def new(i, _):
            r = pl.ds(pl.multiple_of(i * step, step), step)
            total = (keepb[sb, r, :] + recvb[r, :].astype(jnp.float32)).astype(jnp.bfloat16)
            gb[sg, r, :] = total
            gf = total.astype(jnp.float32)
            m1 = 0.9 * mb[r, :] + 0.1 * gf
            v1 = 0.95 * vb[r, :] + 0.05 * gf * gf
            w0 = wb[r, :].astype(jnp.float32)
            nb[sn, r, :] = (w0 - 0.02 * (m1 * lax.rsqrt(v1 + 1e-8) + 0.1 * w0)).astype(jnp.bfloat16)
            return 0

        lax.fori_loop(0, rows // step, new, 0)
        top = pl.ds(0, rows)
        src = nb.at[sn, top, :]
        if inside:
            dst = wn[wi].at[layer, xy, c, rs, :]
            cp.start_remote(("gb", k), src, dst, peer_b)
            if k != late:
                cp.start_remote(("ga", k), src, dst, peer_a)
            cp.start_remote(("mo", k), src, dst, mate)
        else:
            first = layer * m[wi].shape[1] + chunks[k][2]
            i = sum(first >= one for one in firsts) - 1
            dst = own_pieces[i].at[pl.ds(first - firsts[i], rows), :]
            cp.start(("again", k), L_AG + sn, src, own_block.at[pl.ds(first, rows), :])
        cp.start(("wout", k), L_WN + sn, src, dst)
        cp.start(("gout", k), L_G + sg, gb.at[sg, top, :], gs[wi].at[layer, rs, :])

    late = max(k for k in range(count) if chunks[k][0] not in outside)

    def send_late():
        wi, layer, rs, rows, b, _ = at(late)
        cp.start_remote(("ga", late), b[12].at[late % WNEW, pl.ds(0, rows), :], wn[wi].at[layer, xy, c, rs, :], peer_a)
        forward_b(late)

    def when(k, f, gathers=False):
        if 0 <= k < count and not (gathers and (chunks[k][0] in outside or k == late)):
            f(k)

    when(0, exchange)
    when(1, exchange)
    when(0, load_terms)
    for s in range(count + 4 * LAG):
        if s < 2:
            sum_mates(s)
        when(s + 2, exchange)
        when(s + 1, load_terms)
        when(s - LAG, load_a)
        when(s - 2 * LAG, load_b)
        when(s - 3 * LAG, forward_b, True)
        when(s - 4 * LAG, forward_a, True)
        if s >= 2:
            when(s, sum_mates)
        when(s - LAG, sum_a)
        when(s - 2 * LAG, update)
        if s == count - 1:
            send_late()
    forward_a(late)
    cp.drain()


def copy_blocks(a):
    layers, places, cores, r, q = a.shape
    count = layers * places * cores

    def kernel(src, dst, buf, sin, sout):
        def where(i):
            return i // (places * cores), (i // cores) % places, i % cores

        loads = [pltpu.make_async_copy(src.at[where(i)], buf.at[i], sin.at[i]) for i in range(count)]
        stores = [pltpu.make_async_copy(buf.at[i], dst.at[where(i)], sout.at[i]) for i in range(count)]
        for one in loads:
            one.start()
        for one, two in zip(loads, stores):
            one.wait()
            two.start()
        for two in stores:
            two.wait()

    hbm = pl.BlockSpec(memory_space=pl.ANY)
    return pl.pallas_call(
        kernel,
        out_shape=jax.ShapeDtypeStruct(a.shape, a.dtype),
        in_specs=[hbm],
        out_specs=hbm,
        scratch_shapes=[pltpu.VMEM((count, r, q), a.dtype), pltpu.SemaphoreType.DMA((count,)), pltpu.SemaphoreType.DMA((count,))],
        cost_estimate=pl.CostEstimate(flops=4 * 10**9, bytes_accessed=4 * a.size, transcendentals=0),
        compiler_params=pltpu.CompilerParams(vmem_limit_bytes=24 * 2**20),
        name="copy_blocks",
    )(a)


def place_blocks(items, shape, into=None):
    _, _, _, r, q = shape
    jobs = []
    for i, (one, first, place) in enumerate(items):
        done = 0
        while done < one.shape[0]:
            layer, row = divmod(first + done, r)
            take = min(one.shape[0] - done, r - row)
            jobs.append((i, done, layer, row, take, place))
            done += take

    def kernel(*refs):
        dst, sems = refs[-2:]
        me = lax.axis_index("dp")
        x, y, c = me // 4, (me // 2) % 2, me % 2
        stores = []
        for n, (i, done, layer, row, take, place) in enumerate(jobs):
            xy, core = place(x, y, c)
            part = refs[i].at[pl.ds(done, take), :]
            stores.append(pltpu.make_async_copy(part, dst.at[layer, xy, core, pl.ds(row, take), :], sems.at[n]))
        for one in stores:
            one.start()
        for one in stores:
            one.wait()

    hbm = pl.BlockSpec(memory_space=pl.ANY)
    more = [] if into is None else [into]
    return pl.pallas_call(
        kernel,
        out_shape=jax.ShapeDtypeStruct(shape, items[0][0].dtype),
        in_specs=[pl.BlockSpec(memory_space=pltpu.VMEM)] * len(items) + [hbm] * len(more),
        out_specs=hbm,
        scratch_shapes=[pltpu.SemaphoreType.DMA((len(jobs),))],
        input_output_aliases={len(items): 0} if more else {},
        cost_estimate=pl.CostEstimate(flops=10**9, bytes_accessed=4 * q * sum(job[4] for job in jobs), transcendentals=0),
        name="place_blocks",
    )(*[one[0] for one in items], *more)


def gather(own, pieces, firsts, n, shape):
    to_a = [(d, d ^ (2 if d % 2 else 4)) for d in range(n)]
    to_b = [(d, d ^ (4 if d % 2 else 2)) for d in range(n)]
    to_mate = [(d, d ^ 1) for d in range(n)]

    def send(what, pairs):
        got = []
        for one in what:
            got.append(lax.ppermute(one, "dp", pairs))
        return got

    from_b = send(pieces, to_b)
    from_a = send([own], to_a)
    mate_own = send([own], to_mate)
    from_ab = send(from_b, to_a)
    mate_b = send(from_b, to_mate)
    mate_a = send(from_a, to_mate)
    mate_ab = send(from_ab, to_mate)

    def at_x(x, y):
        return 2 * (1 - x) + y

    def at_y(x, y):
        return 2 * x + 1 - y

    def a_of(x, y, c):
        return at_x(x, y) + c * (at_y(x, y) - at_x(x, y))

    def b_of(x, y, c):
        return at_y(x, y) + c * (at_x(x, y) - at_y(x, y))

    def at_own(x, y, c):
        return 2 * x + y, c

    def at_a(x, y, c):
        return a_of(x, y, c), c

    def at_b(x, y, c):
        return b_of(x, y, c), c

    def at_ab(x, y, c):
        return 3 - 2 * x - y, c

    def of_mate(place):
        return lambda x, y, c: place(x, y, 1 - c)

    first, second = firsts
    steps = [
        [(own, 0, at_own), (from_a[0], 0, at_a), (from_b[0], 0, at_b), (mate_own[0], 0, of_mate(at_own)), (mate_b[0], 0, of_mate(at_b))],
        [(from_b[1], second, at_b), (mate_a[0], 0, of_mate(at_a)), (mate_b[1], second, of_mate(at_b))],
        [(from_ab[0], first, at_ab), (mate_ab[0], first, of_mate(at_ab))],
        [(from_ab[1], second, at_ab), (mate_ab[1], second, of_mate(at_ab))],
    ]
    whole = None
    for items in steps:
        whole = place_blocks(items, shape, into=whole)
    return whole


def solution(mesh):
    n = mesh.shape["dp"]

    def inner(*arrays):
        terms, weights, m, v = (arrays[i : i + 3] for i in (0, 3, 6, 9))
        layers = weights[0].shape[0]
        rows = [one.shape[1] for one in m]
        cols = [one.shape[2] for one in m]
        kinds, shapes = [], []
        for one in zip(rows, cols):
            if one not in shapes:
                shapes.append(one)
            kinds.append(shapes.index(one))
        group = [r // 9 for r in rows]
        chunks = chunk_list(rows, 3, layers)

        def blocks(a, r):
            return a.reshape(layers, n // 2, 2, r, a.shape[-1])

        gb = [blocks(t[0], r) for t, r in zip(terms, rows)]
        wb = [blocks(t, r) for t, r in zip(weights, rows)]
        bf, f32 = jnp.bfloat16, jnp.float32
        firsts = (0, layers * rows[2] * 2 // 3)
        ends = (*firsts[1:], layers * rows[2])
        out = [jax.ShapeDtypeStruct((layers * rows[2], cols[2]), bf)]
        out += [jax.ShapeDtypeStruct((end - first, cols[2]), bf) for first, end in zip(firsts, ends)]
        out += [jax.ShapeDtypeStruct((layers, n // 2, 2, r, q), bf) for r, q in zip(rows[:2], cols)]
        out += [jax.ShapeDtypeStruct((layers, r, q), bf) for r, q in zip(rows, cols)]
        out += [jax.ShapeDtypeStruct((layers, n // 2, r, q), bf) for r, q in zip(rows, cols)]
        out += [jax.ShapeDtypeStruct((layers, 2, r, q), bf) for r, q in zip(rows, cols)]
        out += [jax.ShapeDtypeStruct((layers, r, q), bf) for r, q in zip(rows, cols)]
        scratch = []
        for r, q in shapes:
            u = (r // 3, q)
            scratch += [
                pltpu.VMEM((OWN, n // 2, *u), bf),
                pltpu.VMEM((PART, n // 2, *u), bf),
                pltpu.VMEM((SENDA, 2, *u), bf),
                pltpu.VMEM((KEEPA, 2, *u), f32),
                pltpu.VMEM((2, *u), bf),
                pltpu.VMEM((SENDB, *u), bf),
                pltpu.VMEM((KEEPB, *u), f32),
                pltpu.VMEM(u, bf),
                pltpu.VMEM(u, f32),
                pltpu.VMEM(u, f32),
                pltpu.VMEM(u, bf),
                pltpu.VMEM((GOUT, *u), bf),
                pltpu.VMEM((WNEW, *u), bf),
            ]
        wi, _, _, short = chunks[-1]
        scratch += [pltpu.VMEM((2, short, cols[wi]), bf), pltpu.VMEM((short, cols[wi]), bf)]
        copies = 10 * len(chunks)
        scratch += [pltpu.SemaphoreType.DMA((copies,)), pltpu.SemaphoreType.DMA((copies,)), pltpu.SemaphoreType.DMA((L_ALL,))]
        hbm = pl.BlockSpec(memory_space=pl.ANY)
        res = pl.pallas_call(
            functools.partial(body, chunks, group, kinds, (2,), firsts),
            out_shape=out,
            in_specs=[hbm] * 12,
            out_specs=[hbm] * len(out),
            scratch_shapes=scratch,
            compiler_params=pltpu.CompilerParams(collective_id=0, has_side_effects=True, vmem_limit_bytes=60 * 2**20),
            name="sum_step_gather",
        )(*gb, *wb, *m, *v)
        own, pieces, res = res[0], res[1 : 1 + len(firsts)], res[1 + len(firsts) :]
        whole = []
        for one in res[0:2]:
            whole.append(copy_blocks(one))
        whole.append(gather(own, pieces, firsts, n, (layers, n // 2, 2, rows[2], cols[2])))
        whole = [one.reshape(w.shape) for one, w in zip(whole, weights)]
        total = [one.astype(f32) for one in res[2:5]]
        new_m = [0.9 * a + 0.1 * t for a, t in zip(m, total)]
        new_v = [0.95 * a + 0.05 * t * t for a, t in zip(v, total)]
        return (*whole, *new_m, *new_v)

    all_of, cut = P(None, None, None), P(None, "dp", None)
    return jax.shard_map(
        inner,
        mesh=mesh,
        in_specs=(P(("rep", "dp"), None, None, None),) * 3 + (all_of,) * 3 + (cut,) * 6,
        out_specs=(P("rep", None, None),) * 3 + (P("rep", "dp", None),) * 6,
        check_vma=False,
    )
```

```python
import functools

import jax
import jax.numpy as jnp
from jax import lax
from jax.experimental import pallas as pl
from jax.experimental.pallas import tpu as pltpu
from jax.sharding import PartitionSpec as P


MESH = pl.DeviceIdType.MESH
LAG = 2


def chunk_list(rows_of, weights, layers):
    out = []
    pairs = [(w, l) for w in range(weights) for l in range(layers)]
    for i, (w, l) in enumerate(pairs):
        unit = rows_of[w] // 9
        parts = [3, 3, 3]
        if i == 0:
            parts = [1, 2, 3, 3]
        if i == len(pairs) - 1:
            parts = [3, 3, 2, 1]
        first = 0
        for p in parts:
            out.append((w, l, first * unit, p * unit))
            first += p
    return out


TURNS = {"d": 4, "a": 4, "b": 4, "gb": 4, "ga": 6, "gab": 4, "mo": 6, "mb": 6, "mga": 8, "mgab": 8}
FIRST = {kind: sum(list(TURNS.values())[:i]) for i, kind in enumerate(TURNS)}


class Copies:
    def __init__(self, send, recv, local):
        self.send, self.recv, self.local = send, recv, local
        self.remote, self.here = {}, {}

    def start_remote(self, key, src, dst, peer):
        kind, k = key
        before = (kind, k - TURNS[kind])
        self.wait_send(before)
        assert before not in self.remote or not self.remote[before][2]
        n = FIRST[kind] + k % TURNS[kind]
        c = pltpu.make_async_remote_copy(src, dst, self.send.at[n], self.recv.at[n], device_id={"dp": peer}, device_id_type=MESH)
        c.start()
        self.remote[key] = [c, True, True]

    def wait_recv(self, key):
        c = self.remote.get(key)
        if c is not None and c[2]:
            c[0].wait_recv()
            c[2] = False

    def wait_send(self, key):
        c = self.remote.get(key)
        if c is not None and c[1]:
            c[0].wait_send()
            c[1] = False

    def start(self, key, slot, src, dst):
        c = pltpu.make_async_copy(src, dst, self.local.at[slot])
        c.start()
        self.here[key] = c

    def wait(self, key):
        c = self.here.pop(key, None)
        if c is not None:
            c.wait()

    def drain(self):
        for c in self.here.values():
            c.wait()
        for c in self.remote.values():
            if c[1]:
                c[0].wait_send()
            if c[2]:
                c[0].wait_recv()


OWN, PART, SENDA, KEEPA, SENDB, KEEPB, GOUT, WNEW = 2, 2, 3, 3, 2, 3, 2, 4
L_OWN, L_PART, L_RECVA, L_RECVB, L_M, L_V, L_W, L_G, L_WN, L_AG, L_ALL = 0, 2, 4, 5, 6, 7, 8, 9, 11, 15, 19


def body(chunks, group, kinds, outside, firsts, *refs):
    g, w, m, v = refs[0:3], refs[3:6], refs[6:9], refs[9:12]
    own_block, own_pieces, refs = refs[12], refs[13 : 13 + len(firsts)], refs[:12] + refs[13 + len(firsts) :]
    wn, gs, pland, aland, bland = refs[12:14], refs[14:17], refs[17:20], refs[20:23], refs[23:26]
    bufs = (refs[26:39], refs[39:52])
    last_a, last_b, send, recv, local = refs[52:57]

    me = lax.axis_index("dp")
    x, y, c = me // 4, (me // 2) % 2, me % 2
    xy = 2 * x + y
    peer_x, peer_y, mate = me + 4 - 8 * x, me + 2 - 4 * y, me + 1 - 2 * c
    peer_a = peer_x + c * (peer_y - peer_x)
    peer_b = peer_y + c * (peer_x - peer_y)
    xy_x, xy_y = xy + 2 - 4 * x, xy + 1 - 2 * y
    xy_a = xy_x + c * (xy_y - xy_x)
    xy_b = xy_y + c * (xy_x - xy_y)
    xy_ab = 3 - xy

    barrier = pltpu.get_barrier_semaphore()
    for peer in (peer_a, peer_b, mate):
        pl.semaphore_signal(barrier, inc=1, device_id={"dp": peer}, device_id_type=MESH)
    pl.semaphore_wait(barrier, 3)

    cp = Copies(send, recv, local)
    count = len(chunks)

    def at(k):
        wi, layer, first, rows = chunks[k]
        return wi, layer, pl.ds(first, rows), rows, bufs[kinds[wi]], group[wi]

    def exchange(k):
        wi, layer, rs, _, _, _ = at(k)
        land = pland[wi].at[layer, :, rs, :]
        if k < PART:
            land = bufs[kinds[wi]][1].at[k, :, pl.ds(0, chunks[k][3]), :]
        cp.start_remote(("d", k), g[wi].at[layer, :, 1 - c, rs, :], land, mate)

    def load_terms(k):
        wi, layer, rs, rows, b, _ = at(k)
        cp.start(("own", k), L_OWN + k % OWN, g[wi].at[layer, :, c, rs, :], b[0].at[k % OWN, :, pl.ds(0, rows), :])
        cp.wait_recv(("d", k))
        if k >= PART:
            cp.start(("part", k), L_PART + k % PART, pland[wi].at[layer, :, rs, :], b[1].at[k % PART, :, pl.ds(0, rows), :])

    def load_a(k):
        wi, layer, rs, rows, b, _ = at(k)
        cp.wait_recv(("a", k))
        if k == count - 1:
            return
        cp.start(("recva", k), L_RECVA, aland[wi].at[layer, :, rs, :], b[4].at[:, pl.ds(0, rows), :])

    def load_b(k):
        wi, layer, rs, rows, b, _ = at(k)
        top = pl.ds(0, rows)
        cp.start(("m", k), L_M, m[wi].at[layer, rs, :], b[8].at[top, :])
        cp.start(("v", k), L_V, v[wi].at[layer, rs, :], b[9].at[top, :])
        cp.start(("w", k), L_W, w[wi].at[layer, xy, c, rs, :], b[10].at[top, :])
        cp.wait_recv(("b", k))
        if k < count - 1:
            cp.start(("recvb", k), L_RECVB, bland[wi].at[layer, rs, :], b[7].at[top, :])

    def forward_b(k):
        wi, layer, rs, _, _, _ = at(k)
        cp.wait_recv(("gb", k))
        part = wn[wi].at[layer, xy_b, c, rs, :]
        cp.start_remote(("gab", k), part, part, peer_a)
        cp.start_remote(("mb", k), part, part, mate)

    def forward_a(k):
        wi, layer, rs, _, _, _ = at(k)
        for kind, place in (("ga", xy_a), ("gab", xy_ab)):
            cp.wait_recv((kind, k))
            part = wn[wi].at[layer, place, c, rs, :]
            cp.start_remote(("m" + kind, k), part, part, mate)

    def settle(s):
        cp.wait_recv(("mo", s - 3 * LAG))
        cp.wait_recv(("mb", s - 4 * LAG))
        cp.wait_recv(("mga", s - 5 * LAG))
        cp.wait_recv(("mgab", s - 5 * LAG))

    def sum_mates(k):
        wi, layer, rs, rows, b, step = at(k)
        own, part, senda, keepa = b[0], b[1], b[2], b[3]
        cp.wait(("own", k))
        cp.wait(("part", k))
        cp.wait_send(("a", k - SENDA))
        so, sp, ss, sk = k % OWN, k % PART, k % SENDA, k % KEEPA

        def sums(i, _):
            r = pl.ds(pl.multiple_of(i * step, step), step)
            for j, place in ((0, xy_ab), (1, xy_a)):
                t = own[so, place, r, :].astype(jnp.float32) + part[sp, place, r, :].astype(jnp.float32)
                senda[ss, j, r, :] = t.astype(jnp.bfloat16)
            for j, place in ((0, xy_b), (1, xy)):
                t = own[so, place, r, :].astype(jnp.float32) + part[sp, place, r, :].astype(jnp.float32)
                keepa[sk, j, r, :] = t
            return 0

        lax.fori_loop(0, rows // step, sums, 0)
        cp.start_remote(("a", k), senda.at[ss, :, pl.ds(0, rows), :], last_a if k == count - 1 else aland[wi].at[layer, :, rs, :], peer_a)

    def sum_a(k):
        wi, layer, rs, rows, b, step = at(k)
        keepa, recva, sendb, keepb = b[3], b[4], b[5], b[6]
        cp.wait(("recva", k))
        cp.wait_send(("b", k - SENDB))
        sk, ss, sb = k % KEEPA, k % SENDB, k % KEEPB
        recva = last_a if k == count - 1 else recva

        def sums(i, _):
            r = pl.ds(pl.multiple_of(i * step, step), step)
            sendb[ss, r, :] = (keepa[sk, 0, r, :] + recva[0, r, :].astype(jnp.float32)).astype(jnp.bfloat16)
            keepb[sb, r, :] = keepa[sk, 1, r, :] + recva[1, r, :].astype(jnp.float32)
            return 0

        lax.fori_loop(0, rows // step, sums, 0)
        cp.start_remote(("b", k), sendb.at[ss, pl.ds(0, rows), :], last_b if k == count - 1 else bland[wi].at[layer, rs, :], peer_b)

    def update(k):
        wi, layer, rs, rows, b, step = at(k)
        inside = wi not in outside
        keepb, recvb, mb, vb, wb, gb, nb = b[6], b[7], b[8], b[9], b[10], b[11], b[12]
        for kind in ("recvb", "m", "v", "w"):
            cp.wait((kind, k))
        cp.wait(("gout", k - GOUT))
        cp.wait(("wout", k - WNEW))
        cp.wait(("again", k - WNEW))
        for kind in ("gb", "ga", "mo"):
            cp.wait_send((kind, k - WNEW))
        sb, sg, sn = k % KEEPB, k % GOUT, k % WNEW
        recvb = last_b if k == count - 1 else recvb

        def new(i, _):
            r = pl.ds(pl.multiple_of(i * step, step), step)
            total = (keepb[sb, r, :] + recvb[r, :].astype(jnp.float32)).astype(jnp.bfloat16)
            gb[sg, r, :] = total
            gf = total.astype(jnp.float32)
            m1 = 0.9 * mb[r, :] + 0.1 * gf
            v1 = 0.95 * vb[r, :] + 0.05 * gf * gf
            w0 = wb[r, :].astype(jnp.float32)
            nb[sn, r, :] = (w0 - 0.02 * (m1 * lax.rsqrt(v1 + 1e-8) + 0.1 * w0)).astype(jnp.bfloat16)
            return 0

        lax.fori_loop(0, rows // step, new, 0)
        top = pl.ds(0, rows)
        src = nb.at[sn, top, :]
        if inside:
            dst = wn[wi].at[layer, xy, c, rs, :]
            cp.start_remote(("gb", k), src, dst, peer_b)
            if k != late:
                cp.start_remote(("ga", k), src, dst, peer_a)
            cp.start_remote(("mo", k), src, dst, mate)
        else:
            first = layer * m[wi].shape[1] + chunks[k][2]
            i = sum(first >= one for one in firsts) - 1
            dst = own_pieces[i].at[pl.ds(first - firsts[i], rows), :]
            cp.start(("again", k), L_AG + sn, src, own_block.at[pl.ds(first, rows), :])
        cp.start(("wout", k), L_WN + sn, src, dst)
        cp.start(("gout", k), L_G + sg, gb.at[sg, top, :], gs[wi].at[layer, rs, :])

    late = max(k for k in range(count) if chunks[k][0] not in outside)

    def send_late():
        wi, layer, rs, rows, b, _ = at(late)
        cp.start_remote(("ga", late), b[12].at[late % WNEW, pl.ds(0, rows), :], wn[wi].at[layer, xy, c, rs, :], peer_a)
        forward_b(late)

    def when(k, f, gathers=False):
        if 0 <= k < count and not (gathers and (chunks[k][0] in outside or k == late)):
            f(k)

    when(0, exchange)
    when(1, exchange)
    when(0, load_terms)
    for s in range(count + 4 * LAG):
        if s < 2:
            sum_mates(s)
        when(s + 2, exchange)
        when(s + 1, load_terms)
        when(s - LAG, load_a)
        when(s - 2 * LAG, load_b)
        when(s - 3 * LAG, forward_b, True)
        when(s - 4 * LAG, forward_a, True)
        settle(s)
        if s >= 2:
            when(s, sum_mates)
        when(s - LAG, sum_a)
        when(s - 2 * LAG, update)
        if s == count - 1:
            send_late()
    forward_a(late)
    cp.drain()


def copy_blocks(a):
    layers, places, cores, _, _ = a.shape
    count = layers * places * cores

    def kernel(src, dst, sems):
        def where(i):
            return i // (places * cores), (i // cores) % places, i % cores

        stores = [pltpu.make_async_copy(src.at[where(i)], dst.at[where(i)], sems.at[i]) for i in range(count)]
        for one in stores:
            one.start()
        for one in stores:
            one.wait()

    return pl.pallas_call(
        kernel,
        out_shape=jax.ShapeDtypeStruct(a.shape, a.dtype),
        in_specs=[pl.BlockSpec(memory_space=pltpu.VMEM)],
        out_specs=pl.BlockSpec(memory_space=pl.ANY),
        scratch_shapes=[pltpu.SemaphoreType.DMA((count,))],
        cost_estimate=pl.CostEstimate(flops=4 * 10**9, bytes_accessed=4 * a.size, transcendentals=0),
        compiler_params=pltpu.CompilerParams(vmem_limit_bytes=2 * a.size + 2**20),
        name="copy_blocks",
    )(a)


def place_blocks(items, shape, into=None):
    _, _, _, r, q = shape
    jobs = []
    for i, (one, first, place) in enumerate(items):
        done = 0
        while done < one.shape[0]:
            layer, row = divmod(first + done, r)
            take = min(one.shape[0] - done, r - row)
            jobs.append((i, done, layer, row, take, place))
            done += take

    def kernel(*refs):
        dst, sems = refs[-2:]
        me = lax.axis_index("dp")
        x, y, c = me // 4, (me // 2) % 2, me % 2
        stores = []
        for n, (i, done, layer, row, take, place) in enumerate(jobs):
            xy, core = place(x, y, c)
            part = refs[i].at[pl.ds(done, take), :]
            stores.append(pltpu.make_async_copy(part, dst.at[layer, xy, core, pl.ds(row, take), :], sems.at[n]))
        for one in stores:
            one.start()
        for one in stores:
            one.wait()

    hbm = pl.BlockSpec(memory_space=pl.ANY)
    more = [] if into is None else [into]
    return pl.pallas_call(
        kernel,
        out_shape=jax.ShapeDtypeStruct(shape, items[0][0].dtype),
        in_specs=[pl.BlockSpec(memory_space=pltpu.VMEM)] * len(items) + [hbm] * len(more),
        out_specs=hbm,
        scratch_shapes=[pltpu.SemaphoreType.DMA((len(jobs),))],
        input_output_aliases={len(items): 0} if more else {},
        cost_estimate=pl.CostEstimate(flops=10**9, bytes_accessed=4 * q * sum(job[4] for job in jobs), transcendentals=0),
        compiler_params=pltpu.CompilerParams(vmem_limit_bytes=2 * q * sum(job[4] for job in jobs) + 2**20),
        name="place_blocks",
    )(*[one[0] for one in items], *more)


def gather(own, pieces, firsts, n, shape):
    to_a = [(d, d ^ (2 if d % 2 else 4)) for d in range(n)]
    to_b = [(d, d ^ (4 if d % 2 else 2)) for d in range(n)]
    to_mate = [(d, d ^ 1) for d in range(n)]

    def send(what, pairs):
        got = []
        for one in what:
            got.append(lax.ppermute(one, "dp", pairs))
        return got

    from_b = send(pieces, to_b)
    from_a = send([own], to_a)
    mate_own = send([own], to_mate)
    from_ab = send(from_b, to_a)
    mate_b = send(from_b, to_mate)
    mate_a = send(from_a, to_mate)
    mate_ab = send(from_ab, to_mate)

    def at_x(x, y):
        return 2 * (1 - x) + y

    def at_y(x, y):
        return 2 * x + 1 - y

    def a_of(x, y, c):
        return at_x(x, y) + c * (at_y(x, y) - at_x(x, y))

    def b_of(x, y, c):
        return at_y(x, y) + c * (at_x(x, y) - at_y(x, y))

    def at_own(x, y, c):
        return 2 * x + y, c

    def at_a(x, y, c):
        return a_of(x, y, c), c

    def at_b(x, y, c):
        return b_of(x, y, c), c

    def at_ab(x, y, c):
        return 3 - 2 * x - y, c

    def of_mate(place):
        return lambda x, y, c: place(x, y, 1 - c)

    first, second = firsts
    steps = [
        [(own, 0, at_own), (from_a[0], 0, at_a), (from_b[0], 0, at_b), (mate_own[0], 0, of_mate(at_own)), (mate_b[0], 0, of_mate(at_b))],
        [(from_b[1], second, at_b), (mate_a[0], 0, of_mate(at_a)), (mate_b[1], second, of_mate(at_b))],
        [(from_ab[0], first, at_ab), (mate_ab[0], first, of_mate(at_ab))],
        [(from_ab[1], second, at_ab), (mate_ab[1], second, of_mate(at_ab))],
    ]
    whole = None
    for items in steps:
        whole = place_blocks(items, shape, into=whole)
    return whole


def solution(mesh):
    n = mesh.shape["dp"]

    def inner(*arrays):
        terms, weights, m, v = (arrays[i : i + 3] for i in (0, 3, 6, 9))
        layers = weights[0].shape[0]
        rows = [one.shape[1] for one in m]
        cols = [one.shape[2] for one in m]
        kinds, shapes = [], []
        for one in zip(rows, cols):
            if one not in shapes:
                shapes.append(one)
            kinds.append(shapes.index(one))
        group = [r // 9 for r in rows]
        chunks = chunk_list(rows, 3, layers)

        def blocks(a, r):
            return a.reshape(layers, n // 2, 2, r, a.shape[-1])

        gb = [blocks(t[0], r) for t, r in zip(terms, rows)]
        wb = [blocks(t, r) for t, r in zip(weights, rows)]
        bf, f32 = jnp.bfloat16, jnp.float32
        firsts = (0, layers * rows[2] * 2 // 3)
        ends = (*firsts[1:], layers * rows[2])
        out = [jax.ShapeDtypeStruct((layers * rows[2], cols[2]), bf)]
        out += [jax.ShapeDtypeStruct((end - first, cols[2]), bf) for first, end in zip(firsts, ends)]
        out += [jax.ShapeDtypeStruct((layers, n // 2, 2, r, q), bf) for r, q in zip(rows[:2], cols)]
        out += [jax.ShapeDtypeStruct((layers, r, q), bf) for r, q in zip(rows, cols)]
        out += [jax.ShapeDtypeStruct((layers, n // 2, r, q), bf) for r, q in zip(rows, cols)]
        out += [jax.ShapeDtypeStruct((layers, 2, r, q), bf) for r, q in zip(rows, cols)]
        out += [jax.ShapeDtypeStruct((layers, r, q), bf) for r, q in zip(rows, cols)]
        scratch = []
        for r, q in shapes:
            u = (r // 3, q)
            scratch += [
                pltpu.VMEM((OWN, n // 2, *u), bf),
                pltpu.VMEM((PART, n // 2, *u), bf),
                pltpu.VMEM((SENDA, 2, *u), bf),
                pltpu.VMEM((KEEPA, 2, *u), f32),
                pltpu.VMEM((2, *u), bf),
                pltpu.VMEM((SENDB, *u), bf),
                pltpu.VMEM((KEEPB, *u), f32),
                pltpu.VMEM(u, bf),
                pltpu.VMEM(u, f32),
                pltpu.VMEM(u, f32),
                pltpu.VMEM(u, bf),
                pltpu.VMEM((GOUT, *u), bf),
                pltpu.VMEM((WNEW, *u), bf),
            ]
        wi, _, _, short = chunks[-1]
        scratch += [pltpu.VMEM((2, short, cols[wi]), bf), pltpu.VMEM((short, cols[wi]), bf)]
        copies = sum(TURNS.values())
        scratch += [pltpu.SemaphoreType.DMA((copies,)), pltpu.SemaphoreType.DMA((copies,)), pltpu.SemaphoreType.DMA((L_ALL,))]
        hbm = pl.BlockSpec(memory_space=pl.ANY)
        res = pl.pallas_call(
            functools.partial(body, chunks, group, kinds, (2,), firsts),
            out_shape=out,
            in_specs=[hbm] * 12,
            out_specs=[hbm] * len(out),
            scratch_shapes=scratch,
            compiler_params=pltpu.CompilerParams(collective_id=0, has_side_effects=True, vmem_limit_bytes=60 * 2**20),
            name="sum_step_gather",
        )(*gb, *wb, *m, *v)
        own, pieces, res = res[0], res[1 : 1 + len(firsts)], res[1 + len(firsts) :]
        whole = []
        for one in res[0:2]:
            whole.append(copy_blocks(one))
        whole.append(gather(own, pieces, firsts, n, (layers, n // 2, 2, rows[2], cols[2])))
        whole = [one.reshape(w.shape) for one, w in zip(whole, weights)]
        total = [one.astype(f32) for one in res[2:5]]
        new_m = [0.9 * a + 0.1 * t for a, t in zip(m, total)]
        new_v = [0.95 * a + 0.05 * t * t for a, t in zip(v, total)]
        return (*whole, *new_m, *new_v)

    all_of, cut = P(None, None, None), P(None, "dp", None)
    return jax.shard_map(
        inner,
        mesh=mesh,
        in_specs=(P(("rep", "dp"), None, None, None),) * 3 + (all_of,) * 3 + (cut,) * 6,
        out_specs=(P("rep", None, None),) * 3 + (P("rep", "dp", None),) * 6,
        check_vma=False,
    )
```

```python
import functools

import jax
import jax.numpy as jnp
from jax import lax
from jax.experimental import pallas as pl
from jax.experimental.pallas import tpu as pltpu
from jax.sharding import PartitionSpec as P


MESH = pl.DeviceIdType.MESH
LAG = 2


def chunk_list(rows_of, weights, layers):
    out = []
    pairs = [(w, l) for w in range(weights) for l in range(layers)]
    for i, (w, l) in enumerate(pairs):
        unit = rows_of[w] // 9
        parts = [3, 3, 3]
        if i == 0:
            parts = [1, 2, 3, 3]
        if i == len(pairs) - 1:
            parts = [3, 2, 3, 1]
        first = 0
        for p in parts:
            out.append((w, l, first * unit, p * unit))
            first += p
    return out


TURNS = {"d": 4, "a": 4, "b": 4, "gb": 4, "ga": 6, "gab": 4, "mo": 6, "mb": 6, "mga": 8, "mgab": 8, "ah": 2}
FIRST = {kind: sum(list(TURNS.values())[:i]) for i, kind in enumerate(TURNS)}


class Copies:
    def __init__(self, send, recv, local):
        self.send, self.recv, self.local = send, recv, local
        self.remote, self.here = {}, {}

    def start_remote(self, key, src, dst, peer):
        kind, k = key
        before = (kind, k - TURNS[kind])
        self.wait_send(before)
        assert before not in self.remote or not self.remote[before][2]
        n = FIRST[kind] + k % TURNS[kind]
        c = pltpu.make_async_remote_copy(src, dst, self.send.at[n], self.recv.at[n], device_id={"dp": peer}, device_id_type=MESH)
        c.start()
        self.remote[key] = [c, True, True]

    def wait_recv(self, key):
        c = self.remote.get(key)
        if c is not None and c[2]:
            c[0].wait_recv()
            c[2] = False

    def wait_send(self, key):
        c = self.remote.get(key)
        if c is not None and c[1]:
            c[0].wait_send()
            c[1] = False

    def start(self, key, slot, src, dst):
        c = pltpu.make_async_copy(src, dst, self.local.at[slot])
        c.start()
        self.here[key] = c

    def wait(self, key):
        c = self.here.pop(key, None)
        if c is not None:
            c.wait()

    def drain(self):
        for c in self.here.values():
            c.wait()
        for c in self.remote.values():
            if c[1]:
                c[0].wait_send()
            if c[2]:
                c[0].wait_recv()


OWN, PART, SENDA, KEEPA, SENDB, KEEPB, GOUT, WNEW = 2, 2, 3, 3, 2, 3, 2, 4
L_OWN, L_PART, L_RECVA, L_RECVB, L_M, L_V, L_W, L_G, L_WN, L_BLOCK, L_REST, L_ALL = 0, 2, 4, 5, 6, 7, 8, 9, 11, 15, 19, 23


def body(chunks, group, kinds, outside, firsts, ahead, *refs):
    g, w, m, v = refs[0:3], refs[3:6], refs[6:9], refs[9:12]
    from_a, own_block, own_rest = refs[12:15]
    own_pieces, refs = refs[15 : 15 + len(firsts)], refs[:12] + refs[15 + len(firsts) :]
    wn, gs, pland, aland, bland = refs[12:14], refs[14:17], refs[17:20], refs[20:23], refs[23:26]
    bufs = (refs[26:39], refs[39:52])
    last_a, last_b, send, recv, local = refs[52:57]

    me = lax.axis_index("dp")
    x, y, c = me // 4, (me // 2) % 2, me % 2
    xy = 2 * x + y
    peer_x, peer_y, mate = me + 4 - 8 * x, me + 2 - 4 * y, me + 1 - 2 * c
    peer_a = peer_x + c * (peer_y - peer_x)
    peer_b = peer_y + c * (peer_x - peer_y)
    xy_x, xy_y = xy + 2 - 4 * x, xy + 1 - 2 * y
    xy_a = xy_x + c * (xy_y - xy_x)
    xy_b = xy_y + c * (xy_x - xy_y)
    xy_ab = 3 - xy

    barrier = pltpu.get_barrier_semaphore()
    for peer in (peer_a, peer_b, mate):
        pl.semaphore_signal(barrier, inc=1, device_id={"dp": peer}, device_id_type=MESH)
    pl.semaphore_wait(barrier, 3)

    cp = Copies(send, recv, local)
    count = len(chunks)

    def at(k):
        wi, layer, first, rows = chunks[k]
        return wi, layer, pl.ds(first, rows), rows, bufs[kinds[wi]], group[wi]

    def exchange(k):
        wi, layer, rs, _, _, _ = at(k)
        land = pland[wi].at[layer, :, rs, :]
        if k < PART:
            land = bufs[kinds[wi]][1].at[k, :, pl.ds(0, chunks[k][3]), :]
        cp.start_remote(("d", k), g[wi].at[layer, :, 1 - c, rs, :], land, mate)

    def load_terms(k):
        wi, layer, rs, rows, b, _ = at(k)
        cp.start(("own", k), L_OWN + k % OWN, g[wi].at[layer, :, c, rs, :], b[0].at[k % OWN, :, pl.ds(0, rows), :])
        cp.wait_recv(("d", k))
        if k >= PART:
            cp.start(("part", k), L_PART + k % PART, pland[wi].at[layer, :, rs, :], b[1].at[k % PART, :, pl.ds(0, rows), :])

    def load_a(k):
        wi, layer, rs, rows, b, _ = at(k)
        cp.wait_recv(("a", k))
        if k == count - 1:
            return
        cp.start(("recva", k), L_RECVA, aland[wi].at[layer, :, rs, :], b[4].at[:, pl.ds(0, rows), :])

    def load_b(k):
        wi, layer, rs, rows, b, _ = at(k)
        top = pl.ds(0, rows)
        cp.start(("m", k), L_M, m[wi].at[layer, rs, :], b[8].at[top, :])
        cp.start(("v", k), L_V, v[wi].at[layer, rs, :], b[9].at[top, :])
        cp.start(("w", k), L_W, w[wi].at[layer, xy, c, rs, :], b[10].at[top, :])
        cp.wait_recv(("b", k))
        if k < count - 1:
            cp.start(("recvb", k), L_RECVB, bland[wi].at[layer, rs, :], b[7].at[top, :])

    def forward_b(k):
        wi, layer, rs, _, _, _ = at(k)
        cp.wait_recv(("gb", k))
        part = wn[wi].at[layer, xy_b, c, rs, :]
        cp.start_remote(("gab", k), part, part, peer_a)
        cp.start_remote(("mb", k), part, part, mate)

    def forward_a(k):
        wi, layer, rs, _, _, _ = at(k)
        for kind, place in (("ga", xy_a), ("gab", xy_ab)):
            cp.wait_recv((kind, k))
            part = wn[wi].at[layer, place, c, rs, :]
            cp.start_remote(("m" + kind, k), part, part, mate)

    def settle(s):
        cp.wait_recv(("mo", s - 3 * LAG))
        cp.wait_recv(("mb", s - 4 * LAG))
        cp.wait_recv(("mga", s - 5 * LAG))
        cp.wait_recv(("mgab", s - 5 * LAG))

    def sum_mates(k):
        wi, layer, rs, rows, b, step = at(k)
        own, part, senda, keepa = b[0], b[1], b[2], b[3]
        cp.wait(("own", k))
        cp.wait(("part", k))
        cp.wait_send(("a", k - SENDA))
        so, sp, ss, sk = k % OWN, k % PART, k % SENDA, k % KEEPA

        def sums(i, _):
            r = pl.ds(pl.multiple_of(i * step, step), step)
            for j, place in ((0, xy_ab), (1, xy_a)):
                t = own[so, place, r, :].astype(jnp.float32) + part[sp, place, r, :].astype(jnp.float32)
                senda[ss, j, r, :] = t.astype(jnp.bfloat16)
            for j, place in ((0, xy_b), (1, xy)):
                t = own[so, place, r, :].astype(jnp.float32) + part[sp, place, r, :].astype(jnp.float32)
                keepa[sk, j, r, :] = t
            return 0

        lax.fori_loop(0, rows // step, sums, 0)
        cp.start_remote(("a", k), senda.at[ss, :, pl.ds(0, rows), :], last_a if k == count - 1 else aland[wi].at[layer, :, rs, :], peer_a)

    def sum_a(k):
        wi, layer, rs, rows, b, step = at(k)
        keepa, recva, sendb, keepb = b[3], b[4], b[5], b[6]
        cp.wait(("recva", k))
        cp.wait_send(("b", k - SENDB))
        sk, ss, sb = k % KEEPA, k % SENDB, k % KEEPB
        recva = last_a if k == count - 1 else recva

        def sums(i, _):
            r = pl.ds(pl.multiple_of(i * step, step), step)
            sendb[ss, r, :] = (keepa[sk, 0, r, :] + recva[0, r, :].astype(jnp.float32)).astype(jnp.bfloat16)
            keepb[sb, r, :] = keepa[sk, 1, r, :] + recva[1, r, :].astype(jnp.float32)
            return 0

        lax.fori_loop(0, rows // step, sums, 0)
        cp.start_remote(("b", k), sendb.at[ss, pl.ds(0, rows), :], last_b if k == count - 1 else bland[wi].at[layer, rs, :], peer_b)

    def update(k):
        wi, layer, rs, rows, b, step = at(k)
        inside = wi not in outside
        keepb, recvb, mb, vb, wb, gb, nb = b[6], b[7], b[8], b[9], b[10], b[11], b[12]
        for kind in ("recvb", "m", "v", "w"):
            cp.wait((kind, k))
        cp.wait(("gout", k - GOUT))
        cp.wait(("wout", k - WNEW))
        cp.wait(("block", k - WNEW))
        cp.wait(("rest", k - WNEW))
        for kind in ("gb", "ga", "mo"):
            cp.wait_send((kind, k - WNEW))
        sb, sg, sn = k % KEEPB, k % GOUT, k % WNEW
        recvb = last_b if k == count - 1 else recvb

        def new(i, _):
            r = pl.ds(pl.multiple_of(i * step, step), step)
            total = (keepb[sb, r, :] + recvb[r, :].astype(jnp.float32)).astype(jnp.bfloat16)
            gb[sg, r, :] = total
            gf = total.astype(jnp.float32)
            m1 = 0.9 * mb[r, :] + 0.1 * gf
            v1 = 0.95 * vb[r, :] + 0.05 * gf * gf
            w0 = wb[r, :].astype(jnp.float32)
            nb[sn, r, :] = (w0 - 0.02 * (m1 * lax.rsqrt(v1 + 1e-8) + 0.1 * w0)).astype(jnp.bfloat16)
            return 0

        lax.fori_loop(0, rows // step, new, 0)
        top = pl.ds(0, rows)
        src = nb.at[sn, top, :]
        if inside:
            dst = wn[wi].at[layer, xy, c, rs, :]
            cp.start_remote(("gb", k), src, dst, peer_b)
            cp.start_remote(("ga", k), src, dst, peer_a)
            cp.start_remote(("mo", k), src, dst, mate)
        else:
            first = layer * m[wi].shape[1] + chunks[k][2]
            i = sum(first >= one for one in firsts) - 1
            dst = own_pieces[i].at[pl.ds(first - firsts[i], rows), :]
            cp.start(("block", k), L_BLOCK + sn, src, own_block.at[pl.ds(first, rows), :])
            if first >= ahead:
                cp.start(("rest", k), L_REST + sn, src, own_rest.at[pl.ds(first - ahead, rows), :])
        cp.start(("wout", k), L_WN + sn, src, dst)
        cp.start(("gout", k), L_G + sg, gb.at[sg, top, :], gs[wi].at[layer, rs, :])

    def send_ahead():
        for k, (wi, layer, first, rows) in enumerate(chunks):
            row = layer * m[wi].shape[1] + first
            if wi in outside and row < ahead:
                cp.wait(("block", k))
                part = pl.ds(row, rows)
                cp.start_remote(("ah", k), own_block.at[part, :], from_a.at[part, :], peer_a)

    def when(k, f, gathers=False):
        if 0 <= k < count and not (gathers and chunks[k][0] in outside):
            f(k)

    when(0, exchange)
    when(1, exchange)
    when(0, load_terms)
    for s in range(count + 4 * LAG):
        if s < 2:
            sum_mates(s)
        when(s + 2, exchange)
        when(s + 1, load_terms)
        when(s - LAG, load_a)
        when(s - 2 * LAG, load_b)
        when(s - 3 * LAG, forward_b, True)
        when(s - 4 * LAG, forward_a, True)
        settle(s)
        if s >= 2:
            when(s, sum_mates)
        when(s - LAG, sum_a)
        when(s - 2 * LAG, update)
        if s == count - 1:
            send_ahead()
    cp.drain()


def copy_blocks(a):
    layers, places, cores, _, _ = a.shape
    count = layers * places * cores

    def kernel(src, dst, sems):
        def where(i):
            return i // (places * cores), (i // cores) % places, i % cores

        stores = [pltpu.make_async_copy(src.at[where(i)], dst.at[where(i)], sems.at[i]) for i in range(count)]
        for one in stores:
            one.start()
        for one in stores:
            one.wait()

    return pl.pallas_call(
        kernel,
        out_shape=jax.ShapeDtypeStruct(a.shape, a.dtype),
        in_specs=[pl.BlockSpec(memory_space=pltpu.VMEM)],
        out_specs=pl.BlockSpec(memory_space=pl.ANY),
        scratch_shapes=[pltpu.SemaphoreType.DMA((count,))],
        cost_estimate=pl.CostEstimate(flops=4 * 10**9, bytes_accessed=4 * a.size, transcendentals=0),
        compiler_params=pltpu.CompilerParams(vmem_limit_bytes=2 * a.size + 2**20),
        name="copy_blocks",
    )(a)


def place_blocks(items, shape, into=None):
    _, _, _, r, q = shape
    jobs = []
    for i, (one, first, place) in enumerate(items):
        done = 0
        while done < one.shape[0]:
            layer, row = divmod(first + done, r)
            take = min(one.shape[0] - done, r - row)
            jobs.append((i, done, layer, row, take, place))
            done += take

    def kernel(*refs):
        dst, sems = refs[-2:]
        me = lax.axis_index("dp")
        x, y, c = me // 4, (me // 2) % 2, me % 2
        stores = []
        for n, (i, done, layer, row, take, place) in enumerate(jobs):
            xy, core = place(x, y, c)
            part = refs[i].at[pl.ds(done, take), :]
            stores.append(pltpu.make_async_copy(part, dst.at[layer, xy, core, pl.ds(row, take), :], sems.at[n]))
        for one in stores:
            one.start()
        for one in stores:
            one.wait()

    hbm = pl.BlockSpec(memory_space=pl.ANY)
    more = [] if into is None else [into]
    return pl.pallas_call(
        kernel,
        out_shape=jax.ShapeDtypeStruct(shape, items[0][0].dtype),
        in_specs=[pl.BlockSpec(memory_space=pltpu.VMEM)] * len(items) + [hbm] * len(more),
        out_specs=hbm,
        scratch_shapes=[pltpu.SemaphoreType.DMA((len(jobs),))],
        input_output_aliases={len(items): 0} if more else {},
        cost_estimate=pl.CostEstimate(flops=10**9, bytes_accessed=4 * q * sum(job[4] for job in jobs), transcendentals=0),
        compiler_params=pltpu.CompilerParams(vmem_limit_bytes=2 * q * sum(job[4] for job in jobs) + 2**20),
        name="place_blocks",
    )(*[one[0] for one in items], *more)


def gather(own, a_ahead, rest, pieces, firsts, n, shape):
    to_a = [(d, d ^ (2 if d % 2 else 4)) for d in range(n)]
    to_b = [(d, d ^ (4 if d % 2 else 2)) for d in range(n)]
    to_mate = [(d, d ^ 1) for d in range(n)]

    def send(what, pairs):
        got = []
        for one in what:
            got.append(lax.ppermute(one, "dp", pairs))
        return got

    from_b = send(pieces, to_b)
    from_a = [a_ahead] + send([rest], to_a)
    mate_own = send([own], to_mate)
    from_ab = send(from_b, to_a)
    mate_b = send(from_b, to_mate)
    mate_a = send(from_a, to_mate)
    mate_ab = send(from_ab, to_mate)

    def at_x(x, y):
        return 2 * (1 - x) + y

    def at_y(x, y):
        return 2 * x + 1 - y

    def a_of(x, y, c):
        return at_x(x, y) + c * (at_y(x, y) - at_x(x, y))

    def b_of(x, y, c):
        return at_y(x, y) + c * (at_x(x, y) - at_y(x, y))

    def at_own(x, y, c):
        return 2 * x + y, c

    def at_a(x, y, c):
        return a_of(x, y, c), c

    def at_b(x, y, c):
        return b_of(x, y, c), c

    def at_ab(x, y, c):
        return 3 - 2 * x - y, c

    def of_mate(place):
        return lambda x, y, c: place(x, y, 1 - c)

    first, second = firsts
    ahead = a_ahead.shape[0]
    steps = [
        [
            (own, 0, at_own),
            (from_a[0], 0, at_a),
            (from_a[1], ahead, at_a),
            (from_b[0], 0, at_b),
            (mate_own[0], 0, of_mate(at_own)),
            (mate_a[0], 0, of_mate(at_a)),
            (mate_b[0], 0, of_mate(at_b)),
        ],
        [(from_b[1], second, at_b), (mate_a[1], ahead, of_mate(at_a)), (mate_b[1], second, of_mate(at_b))],
        [(from_ab[0], first, at_ab), (mate_ab[0], first, of_mate(at_ab))],
        [(from_ab[1], second, at_ab), (mate_ab[1], second, of_mate(at_ab))],
    ]
    whole = None
    for items in steps:
        whole = place_blocks(items, shape, into=whole)
    return whole


def solution(mesh):
    n = mesh.shape["dp"]

    def inner(*arrays):
        terms, weights, m, v = (arrays[i : i + 3] for i in (0, 3, 6, 9))
        layers = weights[0].shape[0]
        rows = [one.shape[1] for one in m]
        cols = [one.shape[2] for one in m]
        kinds, shapes = [], []
        for one in zip(rows, cols):
            if one not in shapes:
                shapes.append(one)
            kinds.append(shapes.index(one))
        group = [r // 9 for r in rows]
        chunks = chunk_list(rows, 3, layers)

        def blocks(a, r):
            return a.reshape(layers, n // 2, 2, r, a.shape[-1])

        gb = [blocks(t[0], r) for t, r in zip(terms, rows)]
        wb = [blocks(t, r) for t, r in zip(weights, rows)]
        bf, f32 = jnp.bfloat16, jnp.float32
        tall = layers * rows[2]
        firsts, ahead = (0, tall * 7 // 9), tall // 3
        ends = (*firsts[1:], tall)
        out = [jax.ShapeDtypeStruct((r, cols[2]), bf) for r in (ahead, tall, tall - ahead)]
        out += [jax.ShapeDtypeStruct((end - first, cols[2]), bf) for first, end in zip(firsts, ends)]
        out += [jax.ShapeDtypeStruct((layers, n // 2, 2, r, q), bf) for r, q in zip(rows[:2], cols)]
        out += [jax.ShapeDtypeStruct((layers, r, q), bf) for r, q in zip(rows, cols)]
        out += [jax.ShapeDtypeStruct((layers, n // 2, r, q), bf) for r, q in zip(rows, cols)]
        out += [jax.ShapeDtypeStruct((layers, 2, r, q), bf) for r, q in zip(rows, cols)]
        out += [jax.ShapeDtypeStruct((layers, r, q), bf) for r, q in zip(rows, cols)]
        scratch = []
        for r, q in shapes:
            u = (r // 3, q)
            scratch += [
                pltpu.VMEM((OWN, n // 2, *u), bf),
                pltpu.VMEM((PART, n // 2, *u), bf),
                pltpu.VMEM((SENDA, 2, *u), bf),
                pltpu.VMEM((KEEPA, 2, *u), f32),
                pltpu.VMEM((2, *u), bf),
                pltpu.VMEM((SENDB, *u), bf),
                pltpu.VMEM((KEEPB, *u), f32),
                pltpu.VMEM(u, bf),
                pltpu.VMEM(u, f32),
                pltpu.VMEM(u, f32),
                pltpu.VMEM(u, bf),
                pltpu.VMEM((GOUT, *u), bf),
                pltpu.VMEM((WNEW, *u), bf),
            ]
        wi, _, _, short = chunks[-1]
        scratch += [pltpu.VMEM((2, short, cols[wi]), bf), pltpu.VMEM((short, cols[wi]), bf)]
        copies = sum(TURNS.values())
        scratch += [pltpu.SemaphoreType.DMA((copies,)), pltpu.SemaphoreType.DMA((copies,)), pltpu.SemaphoreType.DMA((L_ALL,))]
        hbm = pl.BlockSpec(memory_space=pl.ANY)
        res = pl.pallas_call(
            functools.partial(body, chunks, group, kinds, (2,), firsts, ahead),
            out_shape=out,
            in_specs=[hbm] * 12,
            out_specs=[hbm] * len(out),
            scratch_shapes=scratch,
            compiler_params=pltpu.CompilerParams(collective_id=0, has_side_effects=True, vmem_limit_bytes=60 * 2**20),
            name="sum_step_gather",
        )(*gb, *wb, *m, *v)
        a_ahead, own, rest, pieces, res = *res[:3], res[3 : 3 + len(firsts)], res[3 + len(firsts) :]
        whole = []
        for one in res[0:2]:
            whole.append(copy_blocks(one))
        whole.append(gather(own, a_ahead, rest, pieces, firsts, n, (layers, n // 2, 2, rows[2], cols[2])))
        whole = [one.reshape(w.shape) for one, w in zip(whole, weights)]
        total = [one.astype(f32) for one in res[2:5]]
        new_m = [0.9 * a + 0.1 * t for a, t in zip(m, total)]
        new_v = [0.95 * a + 0.05 * t * t for a, t in zip(v, total)]
        return (*whole, *new_m, *new_v)

    all_of, cut = P(None, None, None), P(None, "dp", None)
    return jax.shard_map(
        inner,
        mesh=mesh,
        in_specs=(P(("rep", "dp"), None, None, None),) * 3 + (all_of,) * 3 + (cut,) * 6,
        out_specs=(P("rep", None, None),) * 3 + (P("rep", "dp", None),) * 6,
        check_vma=False,
    )
```

```python
import functools

import jax
import jax.numpy as jnp
from jax import lax
from jax.experimental import pallas as pl
from jax.experimental.pallas import tpu as pltpu
from jax.sharding import PartitionSpec as P


MESH = pl.DeviceIdType.MESH
LAG = 2


def chunk_list(rows_of, weights, layers):
    out = []
    pairs = [(w, l) for w in range(weights) for l in range(layers)]
    for i, (w, l) in enumerate(pairs):
        unit = rows_of[w] // 9
        parts = [3, 3, 3]
        if i == 0:
            parts = [1, 2, 3, 3]
        if i == len(pairs) - 1:
            parts = [3, 2, 3, 1]
        first = 0
        for p in parts:
            out.append((w, l, first * unit, p * unit))
            first += p
    return out


TURNS = {"d": (3, 4), "a": (3, 4), "b": (2, 4), "gb": (3, 4), "ga": (3, 6), "gab": (3, 4), "mo": (3, 0), "ah": (2, 2), "d0": (4, 4), "a0": (4, 4)}
SLICES = 4
SHARED = 2


def first_of(kind, end):
    return sum(turns[end] for one, turns in list(TURNS.items())[: list(TURNS).index(kind)])


SENDS, RECVS = (sum(turns[end] for turns in TURNS.values()) for end in (0, 1))


class Copies:
    def __init__(self, send, recv, local):
        self.send, self.recv, self.local = send, recv, local
        self.remote, self.here = {}, {}

    def start_remote(self, key, src, dst, peer, shared=None):
        kind, k = key
        sends, recvs = TURNS.get(kind, (0, 0))
        if sends:
            self.wait_send((kind, k - sends))
        before = self.remote.get((kind, k - recvs)) if recvs else None
        assert before is None or not before[2]
        n = first_of(kind, 0) + k % sends if sends else SENDS + shared
        i = first_of(kind, 1) + k % recvs if recvs else RECVS + shared
        c = pltpu.make_async_remote_copy(src, dst, self.send.at[n], self.recv.at[i], device_id={"dp": peer}, device_id_type=MESH)
        c.start()
        self.remote[key] = [c, sends > 0, recvs > 0]

    def wait_shared(self, shared, sent, got, peer):
        c = pltpu.make_async_remote_copy(sent, sent, self.send.at[SENDS + shared], self.recv.at[0], device_id={"dp": peer}, device_id_type=MESH)
        c.wait_send()
        c = pltpu.make_async_remote_copy(got, got, self.send.at[0], self.recv.at[RECVS + shared], device_id={"dp": peer}, device_id_type=MESH)
        c.wait_recv()

    def wait_recv(self, key):
        c = self.remote.get(key)
        if c is not None and c[2]:
            c[0].wait_recv()
            c[2] = False

    def wait_send(self, key):
        c = self.remote.get(key)
        if c is not None and c[1]:
            c[0].wait_send()
            c[1] = False

    def start(self, key, slot, src, dst):
        c = pltpu.make_async_copy(src, dst, self.local.at[slot])
        c.start()
        self.here[key] = c

    def wait(self, key):
        c = self.here.pop(key, None)
        if c is not None:
            c.wait()

    def drain(self):
        for c in self.here.values():
            c.wait()
        for c in self.remote.values():
            if c[1]:
                c[0].wait_send()
            if c[2]:
                c[0].wait_recv()


OWN, PART, SENDA, KEEPA, SENDB, KEEPB, GOUT, WNEW = 2, 2, 3, 3, 2, 3, 2, 4
L_OWN, L_PART, L_RECVA, L_RECVB, L_M, L_V, L_W, L_G, L_WN, L_BLOCK, L_REST, L_ALL = 0, 2, 4, 5, 6, 7, 8, 9, 11, 15, 19, 23


def body(chunks, group, kinds, outside, firsts, ahead, *refs):
    g, w, m, v = refs[0:3], refs[3:6], refs[6:9], refs[9:12]
    from_a, own_block, own_rest = refs[12:15]
    own_pieces, refs = refs[15 : 15 + len(firsts)], refs[:12] + refs[15 + len(firsts) :]
    wn, gs, pland, aland, bland = refs[12:14], refs[14:17], refs[17:20], refs[20:23], refs[23:26]
    bufs = (refs[26:39], refs[39:52])
    last_a, last_b, send, recv, local = refs[52:57]

    me = lax.axis_index("dp")
    x, y, c = me // 4, (me // 2) % 2, me % 2
    xy = 2 * x + y
    peer_x, peer_y, mate = me + 4 - 8 * x, me + 2 - 4 * y, me + 1 - 2 * c
    peer_a = peer_x + c * (peer_y - peer_x)
    peer_b = peer_y + c * (peer_x - peer_y)
    xy_x, xy_y = xy + 2 - 4 * x, xy + 1 - 2 * y
    xy_a = xy_x + c * (xy_y - xy_x)
    xy_b = xy_y + c * (xy_x - xy_y)
    xy_ab = 3 - xy

    barrier = pltpu.get_barrier_semaphore()
    for peer in (peer_a, peer_b, mate):
        pl.semaphore_signal(barrier, inc=1, device_id={"dp": peer}, device_id_type=MESH)
    pl.semaphore_wait(barrier, 3)

    cp = Copies(send, recv, local)
    count = len(chunks)

    def at(k):
        wi, layer, first, rows = chunks[k]
        return wi, layer, pl.ds(first, rows), rows, bufs[kinds[wi]], group[wi]

    def slices(wi):
        width = m[wi].shape[2] // SLICES
        return [pl.ds(i * width, width) for i in range(SLICES)]

    def exchange(k):
        wi, layer, rs, _, _, _ = at(k)
        land = pland[wi].at[layer, :, rs, :]
        if k < PART:
            land = bufs[kinds[wi]][1].at[k, :, pl.ds(0, chunks[k][3]), :]
        if k:
            cp.start_remote(("d", k), g[wi].at[layer, :, 1 - c, rs, :], land, mate)
            return
        for i, part in enumerate(slices(wi)):
            cp.start_remote(("d0", i), g[wi].at[layer, :, 1 - c, rs, part], bufs[kinds[wi]][1].at[k, :, pl.ds(0, chunks[k][3]), part], mate)

    def load_terms(k):
        wi, layer, rs, rows, b, _ = at(k)
        cp.start(("own", k), L_OWN + k % OWN, g[wi].at[layer, :, c, rs, :], b[0].at[k % OWN, :, pl.ds(0, rows), :])
        cp.wait_recv(("d", k))
        if k >= PART:
            cp.start(("part", k), L_PART + k % PART, pland[wi].at[layer, :, rs, :], b[1].at[k % PART, :, pl.ds(0, rows), :])

    def load_a(k):
        wi, layer, rs, rows, b, _ = at(k)
        cp.wait_recv(("a", k))
        if k == 0:
            for i in range(SLICES):
                cp.wait_recv(("a0", i))
        if k == count - 1:
            return
        cp.start(("recva", k), L_RECVA, aland[wi].at[layer, :, rs, :], b[4].at[:, pl.ds(0, rows), :])

    def load_b(k):
        wi, layer, rs, rows, b, _ = at(k)
        top = pl.ds(0, rows)
        cp.start(("m", k), L_M, m[wi].at[layer, rs, :], b[8].at[top, :])
        cp.start(("v", k), L_V, v[wi].at[layer, rs, :], b[9].at[top, :])
        cp.start(("w", k), L_W, w[wi].at[layer, xy, c, rs, :], b[10].at[top, :])
        cp.wait_recv(("b", k))
        if k < count - 1:
            cp.start(("recvb", k), L_RECVB, bland[wi].at[layer, rs, :], b[7].at[top, :])

    def forward_b(k):
        wi, layer, rs, _, _, _ = at(k)
        cp.wait_recv(("gb", k))
        part = wn[wi].at[layer, xy_b, c, rs, :]
        cp.start_remote(("gab", k), part, part, peer_a)
        cp.start_remote(("mb", k), part, part, mate, wi)

    def forward_a(k):
        wi, layer, rs, _, _, _ = at(k)
        for kind, place in (("ga", xy_a), ("gab", xy_ab)):
            cp.wait_recv((kind, k))
            part = wn[wi].at[layer, place, c, rs, :]
            cp.start_remote(("m" + kind, k), part, part, mate, wi)

    def sum_mates(k):
        wi, layer, rs, rows, b, step = at(k)
        own, part, senda, keepa = b[0], b[1], b[2], b[3]
        cp.wait(("own", k))
        cp.wait(("part", k))
        cp.wait_send(("a", k - SENDA))
        if k == SENDA:
            for i in range(SLICES):
                cp.wait_send(("a0", i))
        so, sp, ss, sk = k % OWN, k % PART, k % SENDA, k % KEEPA

        def sums(cols):
            def some(i, _):
                r = pl.ds(pl.multiple_of(i * step, step), step)
                for j, place in ((0, xy_ab), (1, xy_a)):
                    t = own[so, place, r, cols].astype(jnp.float32) + part[sp, place, r, cols].astype(jnp.float32)
                    senda[ss, j, r, cols] = t.astype(jnp.bfloat16)
                for j, place in ((0, xy_b), (1, xy)):
                    t = own[so, place, r, cols].astype(jnp.float32) + part[sp, place, r, cols].astype(jnp.float32)
                    keepa[sk, j, r, cols] = t
                return 0

            lax.fori_loop(0, rows // step, some, 0)

        if k == 0:
            for i, cols in enumerate(slices(wi)):
                cp.wait_recv(("d0", i))
                sums(cols)
                cp.start_remote(("a0", i), senda.at[ss, :, pl.ds(0, rows), cols], aland[wi].at[layer, :, rs, cols], peer_a)
            return
        sums(slice(None))
        cp.start_remote(("a", k), senda.at[ss, :, pl.ds(0, rows), :], last_a if k == count - 1 else aland[wi].at[layer, :, rs, :], peer_a)

    def sum_a(k):
        wi, layer, rs, rows, b, step = at(k)
        keepa, recva, sendb, keepb = b[3], b[4], b[5], b[6]
        cp.wait(("recva", k))
        cp.wait_send(("b", k - SENDB))
        sk, ss, sb = k % KEEPA, k % SENDB, k % KEEPB
        recva = last_a if k == count - 1 else recva

        def sums(i, _):
            r = pl.ds(pl.multiple_of(i * step, step), step)
            sendb[ss, r, :] = (keepa[sk, 0, r, :] + recva[0, r, :].astype(jnp.float32)).astype(jnp.bfloat16)
            keepb[sb, r, :] = keepa[sk, 1, r, :] + recva[1, r, :].astype(jnp.float32)
            return 0

        lax.fori_loop(0, rows // step, sums, 0)
        cp.start_remote(("b", k), sendb.at[ss, pl.ds(0, rows), :], last_b if k == count - 1 else bland[wi].at[layer, rs, :], peer_b)

    def update(k):
        wi, layer, rs, rows, b, step = at(k)
        inside = wi not in outside
        keepb, recvb, mb, vb, wb, gb, nb = b[6], b[7], b[8], b[9], b[10], b[11], b[12]
        for kind in ("recvb", "m", "v", "w"):
            cp.wait((kind, k))
        cp.wait(("gout", k - GOUT))
        cp.wait(("wout", k - WNEW))
        cp.wait(("block", k - WNEW))
        cp.wait(("rest", k - WNEW))
        for kind in ("gb", "ga", "mo"):
            cp.wait_send((kind, k - WNEW))
        sb, sg, sn = k % KEEPB, k % GOUT, k % WNEW
        recvb = last_b if k == count - 1 else recvb

        def new(i, _):
            r = pl.ds(pl.multiple_of(i * step, step), step)
            total = (keepb[sb, r, :] + recvb[r, :].astype(jnp.float32)).astype(jnp.bfloat16)
            gb[sg, r, :] = total
            gf = total.astype(jnp.float32)
            m1 = 0.9 * mb[r, :] + 0.1 * gf
            v1 = 0.95 * vb[r, :] + 0.05 * gf * gf
            w0 = wb[r, :].astype(jnp.float32)
            nb[sn, r, :] = (w0 - 0.02 * (m1 * lax.rsqrt(v1 + 1e-8) + 0.1 * w0)).astype(jnp.bfloat16)
            return 0

        lax.fori_loop(0, rows // step, new, 0)
        top = pl.ds(0, rows)
        src = nb.at[sn, top, :]
        if inside:
            dst = wn[wi].at[layer, xy, c, rs, :]
            cp.start_remote(("gb", k), src, dst, peer_b)
            cp.start_remote(("ga", k), src, dst, peer_a)
            cp.start_remote(("mo", k), src, dst, mate, wi)
        else:
            first = layer * m[wi].shape[1] + chunks[k][2]
            i = sum(first >= one for one in firsts) - 1
            dst = own_pieces[i].at[pl.ds(first - firsts[i], rows), :]
            cp.start(("block", k), L_BLOCK + sn, src, own_block.at[pl.ds(first, rows), :])
            if first >= ahead:
                cp.start(("rest", k), L_REST + sn, src, own_rest.at[pl.ds(first - ahead, rows), :])
        cp.start(("wout", k), L_WN + sn, src, dst)
        cp.start(("gout", k), L_G + sg, gb.at[sg, top, :], gs[wi].at[layer, rs, :])

    def send_ahead():
        for k, (wi, layer, first, rows) in enumerate(chunks):
            row = layer * m[wi].shape[1] + first
            if wi in outside and row < ahead:
                cp.wait(("block", k))
                part = pl.ds(row, rows)
                cp.start_remote(("ah", k), own_block.at[part, :], from_a.at[part, :], peer_a)

    def when(k, f, gathers=False):
        if 0 <= k < count and not (gathers and chunks[k][0] in outside):
            f(k)

    when(0, exchange)
    when(1, exchange)
    when(0, load_terms)
    for s in range(count + 4 * LAG):
        if s < 2:
            sum_mates(s)
        when(s + 2, exchange)
        when(s + 1, load_terms)
        when(s - LAG, load_a)
        when(s - 2 * LAG, load_b)
        when(s - 3 * LAG, forward_b, True)
        when(s - 4 * LAG, forward_a, True)
        if s >= 2:
            when(s, sum_mates)
        when(s - LAG, sum_a)
        when(s - 2 * LAG, update)
        if s == count - 1:
            send_ahead()
    for wi in range(len(wn)):
        cp.wait_shared(wi, wn[wi].at[:, pl.ds(0, 3), c], wn[wi].at[:, :, 1 - c], mate)
    cp.drain()


def copy_blocks(a):
    layers, places, cores, _, _ = a.shape
    count = layers * places * cores

    def kernel(src, dst, sems):
        def where(i):
            return i // (places * cores), (i // cores) % places, i % cores

        stores = [pltpu.make_async_copy(src.at[where(i)], dst.at[where(i)], sems.at[i]) for i in range(count)]
        for one in stores:
            one.start()
        for one in stores:
            one.wait()

    return pl.pallas_call(
        kernel,
        out_shape=jax.ShapeDtypeStruct(a.shape, a.dtype),
        in_specs=[pl.BlockSpec(memory_space=pltpu.VMEM)],
        out_specs=pl.BlockSpec(memory_space=pl.ANY),
        scratch_shapes=[pltpu.SemaphoreType.DMA((count,))],
        cost_estimate=pl.CostEstimate(flops=4 * 10**9, bytes_accessed=4 * a.size, transcendentals=0),
        compiler_params=pltpu.CompilerParams(vmem_limit_bytes=2 * a.size + 2**20),
        name="copy_blocks",
    )(a)


def place_blocks(items, shape, into=None):
    _, _, _, r, q = shape
    jobs = []
    for i, (one, first, place) in enumerate(items):
        done = 0
        while done < one.shape[0]:
            layer, row = divmod(first + done, r)
            take = min(one.shape[0] - done, r - row)
            jobs.append((i, done, layer, row, take, place))
            done += take

    def kernel(*refs):
        dst, sems = refs[-2:]
        me = lax.axis_index("dp")
        x, y, c = me // 4, (me // 2) % 2, me % 2
        stores = []
        for n, (i, done, layer, row, take, place) in enumerate(jobs):
            xy, core = place(x, y, c)
            part = refs[i].at[pl.ds(done, take), :]
            stores.append(pltpu.make_async_copy(part, dst.at[layer, xy, core, pl.ds(row, take), :], sems.at[n]))
        for one in stores:
            one.start()
        for one in stores:
            one.wait()

    hbm = pl.BlockSpec(memory_space=pl.ANY)
    more = [] if into is None else [into]
    return pl.pallas_call(
        kernel,
        out_shape=jax.ShapeDtypeStruct(shape, items[0][0].dtype),
        in_specs=[pl.BlockSpec(memory_space=pltpu.VMEM)] * len(items) + [hbm] * len(more),
        out_specs=hbm,
        scratch_shapes=[pltpu.SemaphoreType.DMA((len(jobs),))],
        input_output_aliases={len(items): 0} if more else {},
        cost_estimate=pl.CostEstimate(flops=10**9, bytes_accessed=4 * q * sum(job[4] for job in jobs), transcendentals=0),
        compiler_params=pltpu.CompilerParams(vmem_limit_bytes=2 * q * sum(job[4] for job in jobs) + 2**20),
        name="place_blocks",
    )(*[one[0] for one in items], *more)


def gather(own, a_ahead, rest, pieces, firsts, n, shape):
    to_a = [(d, d ^ (2 if d % 2 else 4)) for d in range(n)]
    to_b = [(d, d ^ (4 if d % 2 else 2)) for d in range(n)]
    to_mate = [(d, d ^ 1) for d in range(n)]

    def send(what, pairs):
        got = []
        for one in what:
            got.append(lax.ppermute(one, "dp", pairs))
        return got

    from_b = send(pieces, to_b)
    from_a = [a_ahead] + send([rest], to_a)
    mate_own = send([own], to_mate)
    from_ab = send(from_b, to_a)
    mate_b = send(from_b, to_mate)
    mate_a = send(from_a, to_mate)
    mate_ab = send(from_ab, to_mate)

    def at_x(x, y):
        return 2 * (1 - x) + y

    def at_y(x, y):
        return 2 * x + 1 - y

    def a_of(x, y, c):
        return at_x(x, y) + c * (at_y(x, y) - at_x(x, y))

    def b_of(x, y, c):
        return at_y(x, y) + c * (at_x(x, y) - at_y(x, y))

    def at_own(x, y, c):
        return 2 * x + y, c

    def at_a(x, y, c):
        return a_of(x, y, c), c

    def at_b(x, y, c):
        return b_of(x, y, c), c

    def at_ab(x, y, c):
        return 3 - 2 * x - y, c

    def of_mate(place):
        return lambda x, y, c: place(x, y, 1 - c)

    first, second = firsts
    ahead = a_ahead.shape[0]
    steps = [
        [
            (own, 0, at_own),
            (from_a[0], 0, at_a),
            (from_a[1], ahead, at_a),
            (from_b[0], 0, at_b),
            (mate_own[0], 0, of_mate(at_own)),
            (mate_a[0], 0, of_mate(at_a)),
            (mate_b[0], 0, of_mate(at_b)),
        ],
        [(from_b[1], second, at_b), (mate_a[1], ahead, of_mate(at_a)), (mate_b[1], second, of_mate(at_b))],
        [(from_ab[0], first, at_ab), (mate_ab[0], first, of_mate(at_ab))],
        [(from_ab[1], second, at_ab), (mate_ab[1], second, of_mate(at_ab))],
    ]
    whole = None
    for items in steps:
        whole = place_blocks(items, shape, into=whole)
    return whole


def solution(mesh):
    n = mesh.shape["dp"]

    def inner(*arrays):
        terms, weights, m, v = (arrays[i : i + 3] for i in (0, 3, 6, 9))
        layers = weights[0].shape[0]
        rows = [one.shape[1] for one in m]
        cols = [one.shape[2] for one in m]
        kinds, shapes = [], []
        for one in zip(rows, cols):
            if one not in shapes:
                shapes.append(one)
            kinds.append(shapes.index(one))
        group = [r // 9 for r in rows]
        chunks = chunk_list(rows, 3, layers)

        def blocks(a, r):
            return a.reshape(layers, n // 2, 2, r, a.shape[-1])

        gb = [blocks(t[0], r) for t, r in zip(terms, rows)]
        wb = [blocks(t, r) for t, r in zip(weights, rows)]
        bf, f32 = jnp.bfloat16, jnp.float32
        tall = layers * rows[2]
        firsts, ahead = (0, tall * 7 // 9), tall // 3
        ends = (*firsts[1:], tall)
        out = [jax.ShapeDtypeStruct((r, cols[2]), bf) for r in (ahead, tall, tall - ahead)]
        out += [jax.ShapeDtypeStruct((end - first, cols[2]), bf) for first, end in zip(firsts, ends)]
        out += [jax.ShapeDtypeStruct((layers, n // 2, 2, r, q), bf) for r, q in zip(rows[:2], cols)]
        out += [jax.ShapeDtypeStruct((layers, r, q), bf) for r, q in zip(rows, cols)]
        out += [jax.ShapeDtypeStruct((layers, n // 2, r, q), bf) for r, q in zip(rows, cols)]
        out += [jax.ShapeDtypeStruct((layers, 2, r, q), bf) for r, q in zip(rows, cols)]
        out += [jax.ShapeDtypeStruct((layers, r, q), bf) for r, q in zip(rows, cols)]
        scratch = []
        for r, q in shapes:
            u = (r // 3, q)
            scratch += [
                pltpu.VMEM((OWN, n // 2, *u), bf),
                pltpu.VMEM((PART, n // 2, *u), bf),
                pltpu.VMEM((SENDA, 2, *u), bf),
                pltpu.VMEM((KEEPA, 2, *u), f32),
                pltpu.VMEM((2, *u), bf),
                pltpu.VMEM((SENDB, *u), bf),
                pltpu.VMEM((KEEPB, *u), f32),
                pltpu.VMEM(u, bf),
                pltpu.VMEM(u, f32),
                pltpu.VMEM(u, f32),
                pltpu.VMEM(u, bf),
                pltpu.VMEM((GOUT, *u), bf),
                pltpu.VMEM((WNEW, *u), bf),
            ]
        wi, _, _, short = chunks[-1]
        scratch += [pltpu.VMEM((2, short, cols[wi]), bf), pltpu.VMEM((short, cols[wi]), bf)]
        scratch += [pltpu.SemaphoreType.DMA((SENDS + SHARED,)), pltpu.SemaphoreType.DMA((RECVS + SHARED,)), pltpu.SemaphoreType.DMA((L_ALL,))]
        hbm = pl.BlockSpec(memory_space=pl.ANY)
        res = pl.pallas_call(
            functools.partial(body, chunks, group, kinds, (2,), firsts, ahead),
            out_shape=out,
            in_specs=[hbm] * 12,
            out_specs=[hbm] * len(out),
            scratch_shapes=scratch,
            compiler_params=pltpu.CompilerParams(collective_id=0, has_side_effects=True, vmem_limit_bytes=60 * 2**20),
            name="sum_step_gather",
        )(*gb, *wb, *m, *v)
        a_ahead, own, rest, pieces, res = *res[:3], res[3 : 3 + len(firsts)], res[3 + len(firsts) :]
        whole = []
        for one in res[0:2]:
            whole.append(copy_blocks(one))
        whole.append(gather(own, a_ahead, rest, pieces, firsts, n, (layers, n // 2, 2, rows[2], cols[2])))
        whole = [one.reshape(w.shape) for one, w in zip(whole, weights)]
        total = [one.astype(f32) for one in res[2:5]]
        new_m = [0.9 * a + 0.1 * t for a, t in zip(m, total)]
        new_v = [0.95 * a + 0.05 * t * t for a, t in zip(v, total)]
        return (*whole, *new_m, *new_v)

    all_of, cut = P(None, None, None), P(None, "dp", None)
    return jax.shard_map(
        inner,
        mesh=mesh,
        in_specs=(P(("rep", "dp"), None, None, None),) * 3 + (all_of,) * 3 + (cut,) * 6,
        out_specs=(P("rep", None, None),) * 3 + (P("rep", "dp", None),) * 6,
        check_vma=False,
    )
```

```python
import functools

import jax
import jax.numpy as jnp
from jax import lax
from jax.experimental import pallas as pl
from jax.experimental.pallas import tpu as pltpu
from jax.sharding import PartitionSpec as P


MESH = pl.DeviceIdType.MESH
LAG = 2


def chunk_list(rows_of, weights, layers):
    out = []
    pairs = [(w, l) for w in range(weights) for l in range(layers)]
    for i, (w, l) in enumerate(pairs):
        unit = rows_of[w] // 9
        parts = [3, 3, 3]
        if i == 0:
            parts = [1, 2, 3, 3]
        if i == len(pairs) - 1:
            parts = [3, 2, 3, 1]
        first = 0
        for p in parts:
            out.append((w, l, first * unit, p * unit))
            first += p
    return out


TURNS = {"d": (3, 4), "a": (3, 4), "b": (2, 4), "gb": (3, 4), "ga": (3, 6), "gab": (3, 4), "mo": (3, 0), "ah": (2, 2), "d0": (4, 4), "a0": (4, 4)}
SLICES = 4
SHARED = 2


def first_of(kind, end):
    return sum(turns[end] for one, turns in list(TURNS.items())[: list(TURNS).index(kind)])


SENDS, RECVS = (sum(turns[end] for turns in TURNS.values()) for end in (0, 1))


class Copies:
    def __init__(self, send, recv, local):
        self.send, self.recv, self.local = send, recv, local
        self.remote, self.here = {}, {}

    def start_remote(self, key, src, dst, peer, shared=None):
        kind, k = key
        sends, recvs = TURNS.get(kind, (0, 0))
        if sends:
            self.wait_send((kind, k - sends))
        before = self.remote.get((kind, k - recvs)) if recvs else None
        assert before is None or not before[2]
        n = first_of(kind, 0) + k % sends if sends else SENDS + shared
        i = first_of(kind, 1) + k % recvs if recvs else RECVS + shared
        c = pltpu.make_async_remote_copy(src, dst, self.send.at[n], self.recv.at[i], device_id={"dp": peer}, device_id_type=MESH)
        c.start()
        self.remote[key] = [c, sends > 0, recvs > 0]

    def wait_shared(self, shared, sent, got, peer):
        c = pltpu.make_async_remote_copy(sent, sent, self.send.at[SENDS + shared], self.recv.at[0], device_id={"dp": peer}, device_id_type=MESH)
        c.wait_send()
        c = pltpu.make_async_remote_copy(got, got, self.send.at[0], self.recv.at[RECVS + shared], device_id={"dp": peer}, device_id_type=MESH)
        c.wait_recv()

    def wait_recv(self, key):
        c = self.remote.get(key)
        if c is not None and c[2]:
            c[0].wait_recv()
            c[2] = False

    def wait_send(self, key):
        c = self.remote.get(key)
        if c is not None and c[1]:
            c[0].wait_send()
            c[1] = False

    def start(self, key, slot, src, dst):
        c = pltpu.make_async_copy(src, dst, self.local.at[slot])
        c.start()
        self.here[key] = c

    def wait(self, key):
        c = self.here.pop(key, None)
        if c is not None:
            c.wait()

    def drain(self):
        for c in self.here.values():
            c.wait()
        for c in self.remote.values():
            if c[1]:
                c[0].wait_send()
            if c[2]:
                c[0].wait_recv()


OWN, PART, SENDA, KEEPA, SENDB, KEEPB, GOUT, WNEW = 2, 2, 3, 3, 2, 3, 2, 4
L_OWN, L_PART, L_RECVA, L_RECVB, L_M, L_V, L_W, L_G, L_WN, L_BLOCK, L_REST, L_STAGE, L_ALL = 0, 2, 4, 5, 6, 7, 8, 9, 11, 15, 19, 23, 24


def body(chunks, group, kinds, outside, firsts, ahead, *refs):
    g, w, m, v = refs[0:3], refs[3:6], refs[6:9], refs[9:12]
    from_a, own_block, own_rest = refs[12:15]
    own_pieces, refs = refs[15 : 15 + len(firsts)], refs[:12] + refs[15 + len(firsts) :]
    wn, gs, pland, aland, bland = refs[12:14], refs[14:17], refs[17:20], refs[20:23], refs[23:26]
    bufs = (refs[26:39], refs[39:52])
    last_a, last_b, stage, send, recv, local = refs[52:58]

    me = lax.axis_index("dp")
    x, y, c = me // 4, (me // 2) % 2, me % 2
    xy = 2 * x + y
    peer_x, peer_y, mate = me + 4 - 8 * x, me + 2 - 4 * y, me + 1 - 2 * c
    peer_a = peer_x + c * (peer_y - peer_x)
    peer_b = peer_y + c * (peer_x - peer_y)
    xy_x, xy_y = xy + 2 - 4 * x, xy + 1 - 2 * y
    xy_a = xy_x + c * (xy_y - xy_x)
    xy_b = xy_y + c * (xy_x - xy_y)
    xy_ab = 3 - xy

    wi, layer, first, rows = chunks[0]
    early = [
        pltpu.make_async_copy(g[wi].at[layer, :, 1 - c, pl.ds(first, rows), :], stage, local.at[L_STAGE]),
        pltpu.make_async_copy(g[wi].at[layer, :, c, pl.ds(first, rows), :], bufs[kinds[wi]][0].at[0, :, pl.ds(0, rows), :], local.at[L_OWN]),
    ]
    for one in early:
        one.start()

    barrier = pltpu.get_barrier_semaphore()
    for peer in (peer_a, peer_b, mate):
        pl.semaphore_signal(barrier, inc=1, device_id={"dp": peer}, device_id_type=MESH)
    pl.semaphore_wait(barrier, 3)

    cp = Copies(send, recv, local)
    count = len(chunks)

    def at(k):
        wi, layer, first, rows = chunks[k]
        return wi, layer, pl.ds(first, rows), rows, bufs[kinds[wi]], group[wi]

    def slices(wi):
        width = m[wi].shape[2] // SLICES
        return [pl.ds(i * width, width) for i in range(SLICES)]

    def exchange(k):
        wi, layer, rs, _, _, _ = at(k)
        land = pland[wi].at[layer, :, rs, :]
        if k < PART:
            land = bufs[kinds[wi]][1].at[k, :, pl.ds(0, chunks[k][3]), :]
        if k:
            cp.start_remote(("d", k), g[wi].at[layer, :, 1 - c, rs, :], land, mate)
            return
        early[0].wait()
        for i, part in enumerate(slices(wi)):
            cp.start_remote(("d0", i), stage.at[:, :, part], bufs[kinds[wi]][1].at[k, :, pl.ds(0, chunks[k][3]), part], mate)

    def load_terms(k):
        wi, layer, rs, rows, b, _ = at(k)
        if k:
            cp.start(("own", k), L_OWN + k % OWN, g[wi].at[layer, :, c, rs, :], b[0].at[k % OWN, :, pl.ds(0, rows), :])
        cp.wait_recv(("d", k))
        if k >= PART:
            cp.start(("part", k), L_PART + k % PART, pland[wi].at[layer, :, rs, :], b[1].at[k % PART, :, pl.ds(0, rows), :])

    def load_a(k):
        wi, layer, rs, rows, b, _ = at(k)
        cp.wait_recv(("a", k))
        if k == 0:
            for i in range(SLICES):
                cp.wait_recv(("a0", i))
        if k == count - 1:
            return
        cp.start(("recva", k), L_RECVA, aland[wi].at[layer, :, rs, :], b[4].at[:, pl.ds(0, rows), :])

    def load_b(k):
        wi, layer, rs, rows, b, _ = at(k)
        top = pl.ds(0, rows)
        cp.start(("m", k), L_M, m[wi].at[layer, rs, :], b[8].at[top, :])
        cp.start(("v", k), L_V, v[wi].at[layer, rs, :], b[9].at[top, :])
        cp.start(("w", k), L_W, w[wi].at[layer, xy, c, rs, :], b[10].at[top, :])
        cp.wait_recv(("b", k))
        if k < count - 1:
            cp.start(("recvb", k), L_RECVB, bland[wi].at[layer, rs, :], b[7].at[top, :])

    def forward_b(k):
        wi, layer, rs, _, _, _ = at(k)
        cp.wait_recv(("gb", k))
        part = wn[wi].at[layer, xy_b, c, rs, :]
        cp.start_remote(("gab", k), part, part, peer_a)
        cp.start_remote(("mb", k), part, part, mate, wi)

    def forward_a(k):
        wi, layer, rs, _, _, _ = at(k)
        for kind, place in (("ga", xy_a), ("gab", xy_ab)):
            cp.wait_recv((kind, k))
            part = wn[wi].at[layer, place, c, rs, :]
            cp.start_remote(("m" + kind, k), part, part, mate, wi)

    def sum_mates(k):
        wi, layer, rs, rows, b, step = at(k)
        own, part, senda, keepa = b[0], b[1], b[2], b[3]
        cp.wait(("own", k))
        if k == 0:
            early[1].wait()
        cp.wait(("part", k))
        cp.wait_send(("a", k - SENDA))
        if k == SENDA:
            for i in range(SLICES):
                cp.wait_send(("a0", i))
        so, sp, ss, sk = k % OWN, k % PART, k % SENDA, k % KEEPA

        def sums(cols):
            def some(i, _):
                r = pl.ds(pl.multiple_of(i * step, step), step)
                for j, place in ((0, xy_ab), (1, xy_a)):
                    t = own[so, place, r, cols].astype(jnp.float32) + part[sp, place, r, cols].astype(jnp.float32)
                    senda[ss, j, r, cols] = t.astype(jnp.bfloat16)
                for j, place in ((0, xy_b), (1, xy)):
                    t = own[so, place, r, cols].astype(jnp.float32) + part[sp, place, r, cols].astype(jnp.float32)
                    keepa[sk, j, r, cols] = t
                return 0

            lax.fori_loop(0, rows // step, some, 0)

        if k == 0:
            for i, cols in enumerate(slices(wi)):
                cp.wait_recv(("d0", i))
                sums(cols)
                cp.start_remote(("a0", i), senda.at[ss, :, pl.ds(0, rows), cols], aland[wi].at[layer, :, rs, cols], peer_a)
            return
        sums(slice(None))
        cp.start_remote(("a", k), senda.at[ss, :, pl.ds(0, rows), :], last_a if k == count - 1 else aland[wi].at[layer, :, rs, :], peer_a)

    def sum_a(k):
        wi, layer, rs, rows, b, step = at(k)
        keepa, recva, sendb, keepb = b[3], b[4], b[5], b[6]
        cp.wait(("recva", k))
        cp.wait_send(("b", k - SENDB))
        sk, ss, sb = k % KEEPA, k % SENDB, k % KEEPB
        recva = last_a if k == count - 1 else recva

        def sums(i, _):
            r = pl.ds(pl.multiple_of(i * step, step), step)
            sendb[ss, r, :] = (keepa[sk, 0, r, :] + recva[0, r, :].astype(jnp.float32)).astype(jnp.bfloat16)
            keepb[sb, r, :] = keepa[sk, 1, r, :] + recva[1, r, :].astype(jnp.float32)
            return 0

        lax.fori_loop(0, rows // step, sums, 0)
        cp.start_remote(("b", k), sendb.at[ss, pl.ds(0, rows), :], last_b if k == count - 1 else bland[wi].at[layer, rs, :], peer_b)

    def update(k):
        wi, layer, rs, rows, b, step = at(k)
        inside = wi not in outside
        keepb, recvb, mb, vb, wb, gb, nb = b[6], b[7], b[8], b[9], b[10], b[11], b[12]
        for kind in ("recvb", "m", "v", "w"):
            cp.wait((kind, k))
        cp.wait(("gout", k - GOUT))
        cp.wait(("wout", k - WNEW))
        cp.wait(("block", k - WNEW))
        cp.wait(("rest", k - WNEW))
        for kind in ("gb", "ga", "mo"):
            cp.wait_send((kind, k - WNEW))
        sb, sg, sn = k % KEEPB, k % GOUT, k % WNEW
        recvb = last_b if k == count - 1 else recvb

        def new(i, _):
            r = pl.ds(pl.multiple_of(i * step, step), step)
            total = (keepb[sb, r, :] + recvb[r, :].astype(jnp.float32)).astype(jnp.bfloat16)
            gb[sg, r, :] = total
            gf = total.astype(jnp.float32)
            m1 = 0.9 * mb[r, :] + 0.1 * gf
            v1 = 0.95 * vb[r, :] + 0.05 * gf * gf
            w0 = wb[r, :].astype(jnp.float32)
            nb[sn, r, :] = (w0 - 0.02 * (m1 * lax.rsqrt(v1 + 1e-8) + 0.1 * w0)).astype(jnp.bfloat16)
            return 0

        lax.fori_loop(0, rows // step, new, 0)
        top = pl.ds(0, rows)
        src = nb.at[sn, top, :]
        if inside:
            dst = wn[wi].at[layer, xy, c, rs, :]
            cp.start_remote(("gb", k), src, dst, peer_b)
            cp.start_remote(("ga", k), src, dst, peer_a)
            cp.start_remote(("mo", k), src, dst, mate, wi)
        else:
            first = layer * m[wi].shape[1] + chunks[k][2]
            i = sum(first >= one for one in firsts) - 1
            dst = own_pieces[i].at[pl.ds(first - firsts[i], rows), :]
            cp.start(("block", k), L_BLOCK + sn, src, own_block.at[pl.ds(first, rows), :])
            if first >= ahead:
                cp.start(("rest", k), L_REST + sn, src, own_rest.at[pl.ds(first - ahead, rows), :])
        cp.start(("wout", k), L_WN + sn, src, dst)
        cp.start(("gout", k), L_G + sg, gb.at[sg, top, :], gs[wi].at[layer, rs, :])

    def send_ahead():
        for k, (wi, layer, first, rows) in enumerate(chunks):
            row = layer * m[wi].shape[1] + first
            if wi in outside and row < ahead:
                cp.wait(("block", k))
                part = pl.ds(row, rows)
                cp.start_remote(("ah", k), own_block.at[part, :], from_a.at[part, :], peer_a)

    def when(k, f, gathers=False):
        if 0 <= k < count and not (gathers and chunks[k][0] in outside):
            f(k)

    when(0, exchange)
    when(1, exchange)
    when(0, load_terms)
    for s in range(count + 4 * LAG):
        if s < 2:
            sum_mates(s)
        when(s + 2, exchange)
        when(s + 1, load_terms)
        when(s - LAG, load_a)
        when(s - 2 * LAG, load_b)
        when(s - 3 * LAG, forward_b, True)
        when(s - 4 * LAG, forward_a, True)
        if s >= 2:
            when(s, sum_mates)
        when(s - LAG, sum_a)
        when(s - 2 * LAG, update)
        if s == count - 1:
            send_ahead()
    for wi in range(len(wn)):
        cp.wait_shared(wi, wn[wi].at[:, pl.ds(0, 3), c], wn[wi].at[:, :, 1 - c], mate)
    cp.drain()


def copy_blocks(a):
    layers, places, cores, _, _ = a.shape
    count = layers * places * cores

    def kernel(src, dst, sems):
        def where(i):
            return i // (places * cores), (i // cores) % places, i % cores

        stores = [pltpu.make_async_copy(src.at[where(i)], dst.at[where(i)], sems.at[i]) for i in range(count)]
        for one in stores:
            one.start()
        for one in stores:
            one.wait()

    return pl.pallas_call(
        kernel,
        out_shape=jax.ShapeDtypeStruct(a.shape, a.dtype),
        in_specs=[pl.BlockSpec(memory_space=pltpu.VMEM)],
        out_specs=pl.BlockSpec(memory_space=pl.ANY),
        scratch_shapes=[pltpu.SemaphoreType.DMA((count,))],
        cost_estimate=pl.CostEstimate(flops=4 * 10**9, bytes_accessed=4 * a.size, transcendentals=0),
        compiler_params=pltpu.CompilerParams(vmem_limit_bytes=2 * a.size + 2**20),
        name="copy_blocks",
    )(a)


def place_blocks(items, shape, into=None):
    _, _, _, r, q = shape
    jobs = []
    for i, (one, first, place) in enumerate(items):
        done = 0
        while done < one.shape[0]:
            layer, row = divmod(first + done, r)
            take = min(one.shape[0] - done, r - row)
            jobs.append((i, done, layer, row, take, place))
            done += take

    def kernel(*refs):
        dst, sems = refs[-2:]
        me = lax.axis_index("dp")
        x, y, c = me // 4, (me // 2) % 2, me % 2
        stores = []
        for n, (i, done, layer, row, take, place) in enumerate(jobs):
            xy, core = place(x, y, c)
            part = refs[i].at[pl.ds(done, take), :]
            stores.append(pltpu.make_async_copy(part, dst.at[layer, xy, core, pl.ds(row, take), :], sems.at[n]))
        for one in stores:
            one.start()
        for one in stores:
            one.wait()

    hbm = pl.BlockSpec(memory_space=pl.ANY)
    more = [] if into is None else [into]
    return pl.pallas_call(
        kernel,
        out_shape=jax.ShapeDtypeStruct(shape, items[0][0].dtype),
        in_specs=[pl.BlockSpec(memory_space=pltpu.VMEM)] * len(items) + [hbm] * len(more),
        out_specs=hbm,
        scratch_shapes=[pltpu.SemaphoreType.DMA((len(jobs),))],
        input_output_aliases={len(items): 0} if more else {},
        cost_estimate=pl.CostEstimate(flops=10**9, bytes_accessed=4 * q * sum(job[4] for job in jobs), transcendentals=0),
        compiler_params=pltpu.CompilerParams(vmem_limit_bytes=2 * q * sum(job[4] for job in jobs) + 2**20),
        name="place_blocks",
    )(*[one[0] for one in items], *more)


def gather(own, a_ahead, rest, pieces, firsts, n, shape):
    to_a = [(d, d ^ (2 if d % 2 else 4)) for d in range(n)]
    to_b = [(d, d ^ (4 if d % 2 else 2)) for d in range(n)]
    to_mate = [(d, d ^ 1) for d in range(n)]

    def send(what, pairs):
        got = []
        for one in what:
            got.append(lax.ppermute(one, "dp", pairs))
        return got

    from_b = send(pieces, to_b)
    from_a = [a_ahead] + send([rest], to_a)
    mate_own = send([own], to_mate)
    from_ab = send(from_b, to_a)
    mate_b = send(from_b, to_mate)
    mate_a = send(from_a, to_mate)
    mate_ab = send(from_ab, to_mate)

    def at_x(x, y):
        return 2 * (1 - x) + y

    def at_y(x, y):
        return 2 * x + 1 - y

    def a_of(x, y, c):
        return at_x(x, y) + c * (at_y(x, y) - at_x(x, y))

    def b_of(x, y, c):
        return at_y(x, y) + c * (at_x(x, y) - at_y(x, y))

    def at_own(x, y, c):
        return 2 * x + y, c

    def at_a(x, y, c):
        return a_of(x, y, c), c

    def at_b(x, y, c):
        return b_of(x, y, c), c

    def at_ab(x, y, c):
        return 3 - 2 * x - y, c

    def of_mate(place):
        return lambda x, y, c: place(x, y, 1 - c)

    first, second = firsts
    ahead = a_ahead.shape[0]
    steps = [
        [
            (own, 0, at_own),
            (from_a[0], 0, at_a),
            (from_a[1], ahead, at_a),
            (from_b[0], 0, at_b),
            (mate_own[0], 0, of_mate(at_own)),
            (mate_a[0], 0, of_mate(at_a)),
            (mate_b[0], 0, of_mate(at_b)),
        ],
        [(from_b[1], second, at_b), (mate_a[1], ahead, of_mate(at_a)), (mate_b[1], second, of_mate(at_b))],
        [(from_ab[0], first, at_ab), (mate_ab[0], first, of_mate(at_ab))],
        [(from_ab[1], second, at_ab)],
        [(mate_ab[1], second, of_mate(at_ab))],
    ]
    whole = None
    for items in steps:
        whole = place_blocks(items, shape, into=whole)
    return whole


def solution(mesh):
    n = mesh.shape["dp"]

    def inner(*arrays):
        terms, weights, m, v = (arrays[i : i + 3] for i in (0, 3, 6, 9))
        layers = weights[0].shape[0]
        rows = [one.shape[1] for one in m]
        cols = [one.shape[2] for one in m]
        kinds, shapes = [], []
        for one in zip(rows, cols):
            if one not in shapes:
                shapes.append(one)
            kinds.append(shapes.index(one))
        group = [r // 9 for r in rows]
        chunks = chunk_list(rows, 3, layers)

        def blocks(a, r):
            return a.reshape(layers, n // 2, 2, r, a.shape[-1])

        gb = [blocks(t[0], r) for t, r in zip(terms, rows)]
        wb = [blocks(t, r) for t, r in zip(weights, rows)]
        bf, f32 = jnp.bfloat16, jnp.float32
        tall = layers * rows[2]
        firsts, ahead = (0, tall * 7 // 9), tall // 3
        ends = (*firsts[1:], tall)
        out = [jax.ShapeDtypeStruct((r, cols[2]), bf) for r in (ahead, tall, tall - ahead)]
        out += [jax.ShapeDtypeStruct((end - first, cols[2]), bf) for first, end in zip(firsts, ends)]
        out += [jax.ShapeDtypeStruct((layers, n // 2, 2, r, q), bf) for r, q in zip(rows[:2], cols)]
        out += [jax.ShapeDtypeStruct((layers, r, q), bf) for r, q in zip(rows, cols)]
        out += [jax.ShapeDtypeStruct((layers, n // 2, r, q), bf) for r, q in zip(rows, cols)]
        out += [jax.ShapeDtypeStruct((layers, 2, r, q), bf) for r, q in zip(rows, cols)]
        out += [jax.ShapeDtypeStruct((layers, r, q), bf) for r, q in zip(rows, cols)]
        scratch = []
        for r, q in shapes:
            u = (r // 3, q)
            scratch += [
                pltpu.VMEM((OWN, n // 2, *u), bf),
                pltpu.VMEM((PART, n // 2, *u), bf),
                pltpu.VMEM((SENDA, 2, *u), bf),
                pltpu.VMEM((KEEPA, 2, *u), f32),
                pltpu.VMEM((2, *u), bf),
                pltpu.VMEM((SENDB, *u), bf),
                pltpu.VMEM((KEEPB, *u), f32),
                pltpu.VMEM(u, bf),
                pltpu.VMEM(u, f32),
                pltpu.VMEM(u, f32),
                pltpu.VMEM(u, bf),
                pltpu.VMEM((GOUT, *u), bf),
                pltpu.VMEM((WNEW, *u), bf),
            ]
        wi, _, _, short = chunks[-1]
        scratch += [pltpu.VMEM((2, short, cols[wi]), bf), pltpu.VMEM((short, cols[wi]), bf)]
        scratch += [pltpu.VMEM((n // 2, chunks[0][3], cols[chunks[0][0]]), bf)]
        scratch += [pltpu.SemaphoreType.DMA((SENDS + SHARED,)), pltpu.SemaphoreType.DMA((RECVS + SHARED,)), pltpu.SemaphoreType.DMA((L_ALL,))]
        hbm = pl.BlockSpec(memory_space=pl.ANY)
        res = pl.pallas_call(
            functools.partial(body, chunks, group, kinds, (2,), firsts, ahead),
            out_shape=out,
            in_specs=[hbm] * 12,
            out_specs=[hbm] * len(out),
            scratch_shapes=scratch,
            compiler_params=pltpu.CompilerParams(collective_id=0, has_side_effects=True, vmem_limit_bytes=60 * 2**20),
            name="sum_step_gather",
        )(*gb, *wb, *m, *v)
        a_ahead, own, rest, pieces, res = *res[:3], res[3 : 3 + len(firsts)], res[3 + len(firsts) :]
        whole = []
        for one in res[0:2]:
            whole.append(copy_blocks(one))
        whole.append(gather(own, a_ahead, rest, pieces, firsts, n, (layers, n // 2, 2, rows[2], cols[2])))
        whole = [one.reshape(w.shape) for one, w in zip(whole, weights)]
        total = [one.astype(f32) for one in res[2:5]]
        new_m = [0.9 * a + 0.1 * t for a, t in zip(m, total)]
        new_v = [0.95 * a + 0.05 * t * t for a, t in zip(v, total)]
        return (*whole, *new_m, *new_v)

    all_of, cut = P(None, None, None), P(None, "dp", None)
    return jax.shard_map(
        inner,
        mesh=mesh,
        in_specs=(P(("rep", "dp"), None, None, None),) * 3 + (all_of,) * 3 + (cut,) * 6,
        out_specs=(P("rep", None, None),) * 3 + (P("rep", "dp", None),) * 6,
        check_vma=False,
    )
```

```python
import functools

import jax
import jax.numpy as jnp
from jax import lax
from jax.experimental import pallas as pl
from jax.experimental.pallas import tpu as pltpu
from jax.sharding import PartitionSpec as P


MESH = pl.DeviceIdType.MESH
LAG = 2


def chunk_list(rows_of, weights, layers):
    out = []
    pairs = [(w, l) for w in range(weights) for l in range(layers)]
    for i, (w, l) in enumerate(pairs):
        unit = rows_of[w] // 9
        parts = [3, 3, 3]
        if i == 0:
            parts = [1, 2, 3, 3]
        if i == len(pairs) - 1:
            parts = [3, 2, 3, 1]
        first = 0
        for p in parts:
            out.append((w, l, first * unit, p * unit))
            first += p
    return out


TURNS = {"d": (2, 4), "a": (3, 4), "b": (2, 4), "gb": (2, 4), "ga": (2, 6), "gab": (2, 4), "mo": (3, 0), "ah": (2, 2), "d0": (4, 4), "a0": (4, 4)}
SLICES = 4
SHARED = 2


def first_of(kind, end):
    return sum(turns[end] for one, turns in list(TURNS.items())[: list(TURNS).index(kind)])


SENDS, RECVS = (sum(turns[end] for turns in TURNS.values()) for end in (0, 1))


class Copies:
    def __init__(self, send, recv, local):
        self.send, self.recv, self.local = send, recv, local
        self.remote, self.here = {}, {}

    def start_remote(self, key, src, dst, peer, shared=None):
        kind, k = key
        sends, recvs = TURNS.get(kind, (0, 0))
        if sends:
            self.wait_send((kind, k - sends))
        before = self.remote.get((kind, k - recvs)) if recvs else None
        assert before is None or not before[2]
        n = first_of(kind, 0) + k % sends if sends else SENDS + shared
        i = first_of(kind, 1) + k % recvs if recvs else RECVS + shared
        c = pltpu.make_async_remote_copy(src, dst, self.send.at[n], self.recv.at[i], device_id={"dp": peer}, device_id_type=MESH)
        c.start()
        self.remote[key] = [c, sends > 0, recvs > 0]

    def wait_shared(self, shared, sent, got, peer):
        c = pltpu.make_async_remote_copy(sent, sent, self.send.at[SENDS + shared], self.recv.at[0], device_id={"dp": peer}, device_id_type=MESH)
        c.wait_send()
        c = pltpu.make_async_remote_copy(got, got, self.send.at[0], self.recv.at[RECVS + shared], device_id={"dp": peer}, device_id_type=MESH)
        c.wait_recv()

    def wait_recv(self, key):
        c = self.remote.get(key)
        if c is not None and c[2]:
            c[0].wait_recv()
            c[2] = False

    def wait_send(self, key):
        c = self.remote.get(key)
        if c is not None and c[1]:
            c[0].wait_send()
            c[1] = False

    def start(self, key, slot, src, dst):
        c = pltpu.make_async_copy(src, dst, self.local.at[slot])
        c.start()
        self.here[key] = c

    def wait(self, key):
        c = self.here.pop(key, None)
        if c is not None:
            c.wait()

    def drain(self):
        for c in self.here.values():
            c.wait()
        for c in self.remote.values():
            if c[1]:
                c[0].wait_send()
            if c[2]:
                c[0].wait_recv()


OWN, PART, SENDA, KEEPA, SENDB, KEEPB, GOUT, WNEW = 2, 2, 3, 3, 2, 3, 2, 4
L_OWN, L_PART, L_RECVA, L_RECVB, L_M, L_V, L_W, L_G, L_WN, L_BLOCK, L_REST, L_STAGE, L_ALL = 0, 2, 4, 5, 6, 7, 8, 9, 11, 15, 19, 23, 24


def body(chunks, group, kinds, outside, firsts, ahead, *refs):
    g, w, m, v = refs[0:3], refs[3:6], refs[6:9], refs[9:12]
    from_a, own_block, own_rest = refs[12:15]
    own_pieces, refs = refs[15 : 15 + len(firsts)], refs[:12] + refs[15 + len(firsts) :]
    wn, gs, pland, aland, bland = refs[12:14], refs[14:17], refs[17:20], refs[20:23], refs[23:26]
    bufs = (refs[26:39], refs[39:52])
    last_a, last_b, stage, send, recv, local = refs[52:58]

    me = lax.axis_index("dp")
    x, y, c = me // 4, (me // 2) % 2, me % 2
    xy = 2 * x + y
    peer_x, peer_y, mate = me + 4 - 8 * x, me + 2 - 4 * y, me + 1 - 2 * c
    peer_a = peer_x + c * (peer_y - peer_x)
    peer_b = peer_y + c * (peer_x - peer_y)
    xy_x, xy_y = xy + 2 - 4 * x, xy + 1 - 2 * y
    xy_a = xy_x + c * (xy_y - xy_x)
    xy_b = xy_y + c * (xy_x - xy_y)
    xy_ab = 3 - xy

    wi, layer, first, rows = chunks[0]
    early = [
        pltpu.make_async_copy(g[wi].at[layer, :, 1 - c, pl.ds(first, rows), :], stage, local.at[L_STAGE]),
        pltpu.make_async_copy(g[wi].at[layer, :, c, pl.ds(first, rows), :], bufs[kinds[wi]][0].at[0, :, pl.ds(0, rows), :], local.at[L_OWN]),
    ]
    for one in early:
        one.start()

    barrier = pltpu.get_barrier_semaphore()
    for peer in (peer_a, peer_b, mate):
        pl.semaphore_signal(barrier, inc=1, device_id={"dp": peer}, device_id_type=MESH)
    pl.semaphore_wait(barrier, 3)

    cp = Copies(send, recv, local)
    count = len(chunks)

    def at(k):
        wi, layer, first, rows = chunks[k]
        return wi, layer, pl.ds(first, rows), rows, bufs[kinds[wi]], group[wi]

    def slices(wi):
        width = m[wi].shape[2] // SLICES
        return [pl.ds(i * width, width) for i in range(SLICES)]

    def exchange(k):
        wi, layer, rs, _, _, _ = at(k)
        land = pland[wi].at[layer, :, rs, :]
        if k < PART:
            land = bufs[kinds[wi]][1].at[k, :, pl.ds(0, chunks[k][3]), :]
        if k:
            cp.start_remote(("d", k), g[wi].at[layer, :, 1 - c, rs, :], land, mate)
            return
        early[0].wait()
        for i, part in enumerate(slices(wi)):
            cp.start_remote(("d0", i), stage.at[:, :, part], bufs[kinds[wi]][1].at[k, :, pl.ds(0, chunks[k][3]), part], mate)

    def load_terms(k):
        wi, layer, rs, rows, b, _ = at(k)
        if k:
            cp.start(("own", k), L_OWN + k % OWN, g[wi].at[layer, :, c, rs, :], b[0].at[k % OWN, :, pl.ds(0, rows), :])
        cp.wait_recv(("d", k))
        if k >= PART:
            cp.start(("part", k), L_PART + k % PART, pland[wi].at[layer, :, rs, :], b[1].at[k % PART, :, pl.ds(0, rows), :])

    def load_a(k):
        wi, layer, rs, rows, b, _ = at(k)
        cp.wait_recv(("a", k))
        if k == 0:
            for i in range(SLICES):
                cp.wait_recv(("a0", i))
        if k == count - 1:
            return
        cp.start(("recva", k), L_RECVA, aland[wi].at[layer, :, rs, :], b[4].at[:, pl.ds(0, rows), :])

    def load_b(k):
        wi, layer, rs, rows, b, _ = at(k)
        top = pl.ds(0, rows)
        cp.start(("m", k), L_M, m[wi].at[layer, rs, :], b[8].at[top, :])
        cp.start(("v", k), L_V, v[wi].at[layer, rs, :], b[9].at[top, :])
        cp.start(("w", k), L_W, w[wi].at[layer, xy, c, rs, :], b[10].at[top, :])
        cp.wait_recv(("b", k))
        if k < count - 1:
            cp.start(("recvb", k), L_RECVB, bland[wi].at[layer, rs, :], b[7].at[top, :])

    def forward_b(k):
        wi, layer, rs, _, _, _ = at(k)
        cp.wait_recv(("gb", k))
        part = wn[wi].at[layer, xy_b, c, rs, :]
        cp.start_remote(("gab", k), part, part, peer_a)
        cp.start_remote(("mb", k), part, part, mate, wi)

    def forward_a(k):
        wi, layer, rs, _, _, _ = at(k)
        for kind, place in (("ga", xy_a), ("gab", xy_ab)):
            cp.wait_recv((kind, k))
            part = wn[wi].at[layer, place, c, rs, :]
            cp.start_remote(("m" + kind, k), part, part, mate, wi)

    def sum_mates(k):
        wi, layer, rs, rows, b, step = at(k)
        own, part, senda, keepa = b[0], b[1], b[2], b[3]
        cp.wait(("own", k))
        if k == 0:
            early[1].wait()
        cp.wait(("part", k))
        cp.wait_send(("a", k - SENDA))
        if k == SENDA:
            for i in range(SLICES):
                cp.wait_send(("a0", i))
        so, sp, ss, sk = k % OWN, k % PART, k % SENDA, k % KEEPA

        def sums(cols):
            def some(i, _):
                r = pl.ds(pl.multiple_of(i * step, step), step)
                for j, place in ((0, xy_ab), (1, xy_a)):
                    t = own[so, place, r, cols].astype(jnp.float32) + part[sp, place, r, cols].astype(jnp.float32)
                    senda[ss, j, r, cols] = t.astype(jnp.bfloat16)
                for j, place in ((0, xy_b), (1, xy)):
                    t = own[so, place, r, cols].astype(jnp.float32) + part[sp, place, r, cols].astype(jnp.float32)
                    keepa[sk, j, r, cols] = t
                return 0

            lax.fori_loop(0, rows // step, some, 0)

        if k == 0:
            for i, cols in enumerate(slices(wi)):
                cp.wait_recv(("d0", i))
                sums(cols)
                cp.start_remote(("a0", i), senda.at[ss, :, pl.ds(0, rows), cols], aland[wi].at[layer, :, rs, cols], peer_a)
            return
        sums(slice(None))
        cp.start_remote(("a", k), senda.at[ss, :, pl.ds(0, rows), :], last_a if k == count - 1 else aland[wi].at[layer, :, rs, :], peer_a)

    def sum_a(k):
        wi, layer, rs, rows, b, step = at(k)
        keepa, recva, sendb, keepb = b[3], b[4], b[5], b[6]
        cp.wait(("recva", k))
        cp.wait_send(("b", k - SENDB))
        sk, ss, sb = k % KEEPA, k % SENDB, k % KEEPB
        recva = last_a if k == count - 1 else recva

        def sums(i, _):
            r = pl.ds(pl.multiple_of(i * step, step), step)
            sendb[ss, r, :] = (keepa[sk, 0, r, :] + recva[0, r, :].astype(jnp.float32)).astype(jnp.bfloat16)
            keepb[sb, r, :] = keepa[sk, 1, r, :] + recva[1, r, :].astype(jnp.float32)
            return 0

        lax.fori_loop(0, rows // step, sums, 0)
        cp.start_remote(("b", k), sendb.at[ss, pl.ds(0, rows), :], last_b if k == count - 1 else bland[wi].at[layer, rs, :], peer_b)

    def update(k):
        wi, layer, rs, rows, b, step = at(k)
        inside = wi not in outside
        keepb, recvb, mb, vb, wb, gb, nb = b[6], b[7], b[8], b[9], b[10], b[11], b[12]
        for kind in ("recvb", "m", "v", "w"):
            cp.wait((kind, k))
        cp.wait(("gout", k - GOUT))
        cp.wait(("wout", k - WNEW))
        cp.wait(("block", k - WNEW))
        cp.wait(("rest", k - WNEW))
        for kind in ("gb", "ga", "mo"):
            cp.wait_send((kind, k - WNEW))
        sb, sg, sn = k % KEEPB, k % GOUT, k % WNEW
        recvb = last_b if k == count - 1 else recvb

        def new(i, _):
            r = pl.ds(pl.multiple_of(i * step, step), step)
            total = (keepb[sb, r, :] + recvb[r, :].astype(jnp.float32)).astype(jnp.bfloat16)
            gb[sg, r, :] = total
            gf = total.astype(jnp.float32)
            m1 = 0.9 * mb[r, :] + 0.1 * gf
            v1 = 0.95 * vb[r, :] + 0.05 * gf * gf
            w0 = wb[r, :].astype(jnp.float32)
            nb[sn, r, :] = (w0 - 0.02 * (m1 * lax.rsqrt(v1 + 1e-8) + 0.1 * w0)).astype(jnp.bfloat16)
            return 0

        lax.fori_loop(0, rows // step, new, 0)
        top = pl.ds(0, rows)
        src = nb.at[sn, top, :]
        if inside:
            dst = wn[wi].at[layer, xy, c, rs, :]
            cp.start_remote(("gb", k), src, dst, peer_b)
            cp.start_remote(("ga", k), src, dst, peer_a)
            cp.start_remote(("mo", k), src, dst, mate, wi)
        else:
            first = layer * m[wi].shape[1] + chunks[k][2]
            i = sum(first >= one for one in firsts) - 1
            dst = own_pieces[i].at[pl.ds(first - firsts[i], rows), :]
            cp.start(("block", k), L_BLOCK + sn, src, own_block.at[pl.ds(first, rows), :])
            if first >= ahead:
                cp.start(("rest", k), L_REST + sn, src, own_rest.at[pl.ds(first - ahead, rows), :])
        cp.start(("wout", k), L_WN + sn, src, dst)
        cp.start(("gout", k), L_G + sg, gb.at[sg, top, :], gs[wi].at[layer, rs, :])

    def send_ahead():
        for k, (wi, layer, first, rows) in enumerate(chunks):
            row = layer * m[wi].shape[1] + first
            if wi in outside and row < ahead:
                cp.wait(("block", k))
                part = pl.ds(row, rows)
                cp.start_remote(("ah", k), own_block.at[part, :], from_a.at[part, :], peer_a)

    def when(k, f, gathers=False):
        if 0 <= k < count and not (gathers and chunks[k][0] in outside):
            f(k)

    when(0, exchange)
    when(1, exchange)
    when(0, load_terms)
    for s in range(count + 4 * LAG):
        if s < 2:
            sum_mates(s)
        when(s + 2, exchange)
        when(s + 1, load_terms)
        when(s - LAG, load_a)
        when(s - 2 * LAG, load_b)
        when(s - 3 * LAG, forward_b, True)
        when(s - 4 * LAG, forward_a, True)
        if s >= 2:
            when(s, sum_mates)
        when(s - LAG, sum_a)
        when(s - 2 * LAG, update)
        if s == count - 1:
            send_ahead()
    for wi in range(len(wn)):
        cp.wait_shared(wi, wn[wi].at[:, pl.ds(0, 3), c], wn[wi].at[:, :, 1 - c], mate)
    cp.drain()


def copy_blocks(a):
    layers, places, cores, _, _ = a.shape
    count = layers * places * cores

    def kernel(src, dst, sems):
        def where(i):
            return i // (places * cores), (i // cores) % places, i % cores

        stores = [pltpu.make_async_copy(src.at[where(i)], dst.at[where(i)], sems.at[i]) for i in range(count)]
        for one in stores:
            one.start()
        for one in stores:
            one.wait()

    return pl.pallas_call(
        kernel,
        out_shape=jax.ShapeDtypeStruct(a.shape, a.dtype),
        in_specs=[pl.BlockSpec(memory_space=pltpu.VMEM)],
        out_specs=pl.BlockSpec(memory_space=pl.ANY),
        scratch_shapes=[pltpu.SemaphoreType.DMA((count,))],
        cost_estimate=pl.CostEstimate(flops=4 * 10**9, bytes_accessed=4 * a.size, transcendentals=0),
        compiler_params=pltpu.CompilerParams(vmem_limit_bytes=2 * a.size + 2**20),
        name="copy_blocks",
    )(a)


def place_blocks(items, shape, into=None):
    _, _, _, r, q = shape
    jobs = []
    for i, (one, first, place) in enumerate(items):
        done = 0
        while done < one.shape[0]:
            layer, row = divmod(first + done, r)
            take = min(one.shape[0] - done, r - row)
            jobs.append((i, done, layer, row, take, place))
            done += take

    def kernel(*refs):
        dst, sems = refs[-2:]
        me = lax.axis_index("dp")
        x, y, c = me // 4, (me // 2) % 2, me % 2
        stores = []
        for n, (i, done, layer, row, take, place) in enumerate(jobs):
            xy, core = place(x, y, c)
            part = refs[i].at[pl.ds(done, take), :]
            stores.append(pltpu.make_async_copy(part, dst.at[layer, xy, core, pl.ds(row, take), :], sems.at[n]))
        for one in stores:
            one.start()
        for one in stores:
            one.wait()

    hbm = pl.BlockSpec(memory_space=pl.ANY)
    more = [] if into is None else [into]
    return pl.pallas_call(
        kernel,
        out_shape=jax.ShapeDtypeStruct(shape, items[0][0].dtype),
        in_specs=[pl.BlockSpec(memory_space=pltpu.VMEM)] * len(items) + [hbm] * len(more),
        out_specs=hbm,
        scratch_shapes=[pltpu.SemaphoreType.DMA((len(jobs),))],
        input_output_aliases={len(items): 0} if more else {},
        cost_estimate=pl.CostEstimate(flops=10**9, bytes_accessed=4 * q * sum(job[4] for job in jobs), transcendentals=0),
        compiler_params=pltpu.CompilerParams(vmem_limit_bytes=2 * q * sum(job[4] for job in jobs) + 2**20),
        name="place_blocks",
    )(*[one[0] for one in items], *more)


def gather(own, a_ahead, rest, pieces, firsts, n, shape):
    to_a = [(d, d ^ (2 if d % 2 else 4)) for d in range(n)]
    to_b = [(d, d ^ (4 if d % 2 else 2)) for d in range(n)]
    to_mate = [(d, d ^ 1) for d in range(n)]

    def send(what, pairs):
        got = []
        for one in what:
            got.append(lax.ppermute(one, "dp", pairs))
        return got

    from_b = send(pieces, to_b)
    from_a = [a_ahead] + send([rest], to_a)
    mate_own = send([own], to_mate)
    from_ab = send(from_b, to_a)
    mate_b = send(from_b, to_mate)
    mate_a = send(from_a, to_mate)
    mate_ab = send(from_ab, to_mate)

    def at_x(x, y):
        return 2 * (1 - x) + y

    def at_y(x, y):
        return 2 * x + 1 - y

    def a_of(x, y, c):
        return at_x(x, y) + c * (at_y(x, y) - at_x(x, y))

    def b_of(x, y, c):
        return at_y(x, y) + c * (at_x(x, y) - at_y(x, y))

    def at_own(x, y, c):
        return 2 * x + y, c

    def at_a(x, y, c):
        return a_of(x, y, c), c

    def at_b(x, y, c):
        return b_of(x, y, c), c

    def at_ab(x, y, c):
        return 3 - 2 * x - y, c

    def of_mate(place):
        return lambda x, y, c: place(x, y, 1 - c)

    first, second = firsts
    ahead = a_ahead.shape[0]
    steps = [
        [
            (own, 0, at_own),
            (from_a[0], 0, at_a),
            (from_a[1], ahead, at_a),
            (from_b[0], 0, at_b),
            (mate_own[0], 0, of_mate(at_own)),
            (mate_a[0], 0, of_mate(at_a)),
            (mate_b[0], 0, of_mate(at_b)),
        ],
        [(from_b[1], second, at_b), (mate_a[1], ahead, of_mate(at_a)), (mate_b[1], second, of_mate(at_b))],
        [(from_ab[0], first, at_ab)],
        [(mate_ab[0], first, of_mate(at_ab))],
        [(from_ab[1], second, at_ab)],
        [(mate_ab[1], second, of_mate(at_ab))],
    ]
    whole = None
    for items in steps:
        whole = place_blocks(items, shape, into=whole)
    return whole


def solution(mesh):
    n = mesh.shape["dp"]

    def inner(*arrays):
        terms, weights, m, v = (arrays[i : i + 3] for i in (0, 3, 6, 9))
        layers = weights[0].shape[0]
        rows = [one.shape[1] for one in m]
        cols = [one.shape[2] for one in m]
        kinds, shapes = [], []
        for one in zip(rows, cols):
            if one not in shapes:
                shapes.append(one)
            kinds.append(shapes.index(one))
        group = [r // 9 for r in rows]
        chunks = chunk_list(rows, 3, layers)

        def blocks(a, r):
            return a.reshape(layers, n // 2, 2, r, a.shape[-1])

        gb = [blocks(t[0], r) for t, r in zip(terms, rows)]
        wb = [blocks(t, r) for t, r in zip(weights, rows)]
        bf, f32 = jnp.bfloat16, jnp.float32
        tall = layers * rows[2]
        firsts, ahead = (0, tall * 7 // 9), tall // 3
        ends = (*firsts[1:], tall)
        out = [jax.ShapeDtypeStruct((r, cols[2]), bf) for r in (ahead, tall, tall - ahead)]
        out += [jax.ShapeDtypeStruct((end - first, cols[2]), bf) for first, end in zip(firsts, ends)]
        out += [jax.ShapeDtypeStruct((layers, n // 2, 2, r, q), bf) for r, q in zip(rows[:2], cols)]
        out += [jax.ShapeDtypeStruct((layers, r, q), bf) for r, q in zip(rows, cols)]
        out += [jax.ShapeDtypeStruct((layers, n // 2, r, q), bf) for r, q in zip(rows, cols)]
        out += [jax.ShapeDtypeStruct((layers, 2, r, q), bf) for r, q in zip(rows, cols)]
        out += [jax.ShapeDtypeStruct((layers, r, q), bf) for r, q in zip(rows, cols)]
        scratch = []
        for r, q in shapes:
            u = (r // 3, q)
            scratch += [
                pltpu.VMEM((OWN, n // 2, *u), bf),
                pltpu.VMEM((PART, n // 2, *u), bf),
                pltpu.VMEM((SENDA, 2, *u), bf),
                pltpu.VMEM((KEEPA, 2, *u), f32),
                pltpu.VMEM((2, *u), bf),
                pltpu.VMEM((SENDB, *u), bf),
                pltpu.VMEM((KEEPB, *u), f32),
                pltpu.VMEM(u, bf),
                pltpu.VMEM(u, f32),
                pltpu.VMEM(u, f32),
                pltpu.VMEM(u, bf),
                pltpu.VMEM((GOUT, *u), bf),
                pltpu.VMEM((WNEW, *u), bf),
            ]
        wi, _, _, short = chunks[-1]
        scratch += [pltpu.VMEM((2, short, cols[wi]), bf), pltpu.VMEM((short, cols[wi]), bf)]
        scratch += [pltpu.VMEM((n // 2, chunks[0][3], cols[chunks[0][0]]), bf)]
        scratch += [pltpu.SemaphoreType.DMA((SENDS + SHARED,)), pltpu.SemaphoreType.DMA((RECVS + SHARED,)), pltpu.SemaphoreType.DMA((L_ALL,))]
        hbm = pl.BlockSpec(memory_space=pl.ANY)
        res = pl.pallas_call(
            functools.partial(body, chunks, group, kinds, (2,), firsts, ahead),
            out_shape=out,
            in_specs=[hbm] * 12,
            out_specs=[hbm] * len(out),
            scratch_shapes=scratch,
            compiler_params=pltpu.CompilerParams(collective_id=0, has_side_effects=True, vmem_limit_bytes=60 * 2**20),
            name="sum_step_gather",
        )(*gb, *wb, *m, *v)
        a_ahead, own, rest, pieces, res = *res[:3], res[3 : 3 + len(firsts)], res[3 + len(firsts) :]
        whole = []
        for one in res[0:2]:
            whole.append(copy_blocks(one))
        whole.append(gather(own, a_ahead, rest, pieces, firsts, n, (layers, n // 2, 2, rows[2], cols[2])))
        whole = [one.reshape(w.shape) for one, w in zip(whole, weights)]
        total = [one.astype(f32) for one in res[2:5]]
        new_m = [0.9 * a + 0.1 * t for a, t in zip(m, total)]
        new_v = [0.95 * a + 0.05 * t * t for a, t in zip(v, total)]
        return (*whole, *new_m, *new_v)

    all_of, cut = P(None, None, None), P(None, "dp", None)
    return jax.shard_map(
        inner,
        mesh=mesh,
        in_specs=(P(("rep", "dp"), None, None, None),) * 3 + (all_of,) * 3 + (cut,) * 6,
        out_specs=(P("rep", None, None),) * 3 + (P("rep", "dp", None),) * 6,
        check_vma=False,
    )
```
